128 devices in a mesh: grp: 4 (over x), dp: 32 (over y, z, core).
Axes of the slice: x: 4, y: 4, z: 4, core: 2. Of those that a mesh axis runs over, the one named last changes fastest.
Arguments:
- inputs: bfloat16 [49152, 2048], P(('grp', 'dp')), may hold values from -6 to 6
- upstream: bfloat16 [49152, 2048], P(('grp', 'dp')), may hold values from -18 to 18
- doc_ids: int32 [49152], P(('grp', 'dp')), may hold values from 0 to 1023, never falling along the last dimension, each value on 1 to 128 neighbouring positions
- qkv_weight: float32 [2048, 3072], P(('grp', 'dp')), may hold values from -8 to 8
- out_weight: float32 [2048, 2048], P(('grp', 'dp')), may hold values from -0.125 to 0.125
- qkv_mean: float32 [2048, 3072], P(('grp', 'dp')), may hold values from -3 to 3
- qkv_square: float32 [2048, 3072], P(('grp', 'dp')), may hold values from 0.3 to 3
- out_mean: float32 [2048, 2048], P(('grp', 'dp')), may hold values from -3 to 3
- out_square: float32 [2048, 2048], P(('grp', 'dp')), may hold values from 0.3 to 3
Outputs:
- attn_out: bfloat16 [49152, 2048], P(('grp', 'dp'))
- new_qkv_weight: float32 [2048, 3072], P(('grp', 'dp'))
- new_out_weight: float32 [2048, 2048], P(('grp', 'dp'))
- new_qkv_mean: float32 [2048, 3072], P(('grp', 'dp'))
- new_qkv_square: float32 [2048, 3072], P(('grp', 'dp'))
- new_out_mean: float32 [2048, 2048], P(('grp', 'dp'))
- new_out_square: float32 [2048, 2048], P(('grp', 'dp'))
The draws below stay inside these ranges and needn't reach their ends.
All inputs are finite; a program needn't handle non-finite values.
Results may differ from the reference program's by a relative error of at most 0.0075.
The reference program's roundings to bfloat16 on the way count: a program that leaves them out, or rounds other values in their place, can miss the bound.
Values may be sent and summed in bfloat16 or wider, within the bound.
No kernel may reach another device: no remote copies, remote signals or barrier semaphores. Data moves between devices by JAX's collectives and lax.ppermute only.
A program may use at most 128 MiB of HBM per device.

```python
import math
import jax
import jax.numpy as jnp
import numpy as np
from jax import lax

D = 2048
QH = 16
KVH = 4
HD = 128
TOK_DEV = 384
TOKENS = 49152
QKV_COLS = 3072
N_GRP = 4
N_DP = 32


def draw_inputs(key, part):
    first_key = jax.random.fold_in(jax.random.fold_in(key, 11), 0)
    entries = jax.random.normal(first_key, (TOKENS, D), jnp.float32)
    column_share = jnp.arange(D).astype(jnp.float32) / (D - 1)
    column_scales = 1.0 + 2.0 * column_share
    entries = entries * column_scales[None, :]
    return jnp.clip(entries, -6.0, 6.0).astype(jnp.bfloat16)


def draw_upstream(key, part):
    first_key = jax.random.fold_in(key, 37)
    holders = TOKENS // TOK_DEV
    holder = (jnp.arange(TOKENS) // TOK_DEV).astype(jnp.float32)
    share = holder / max(holders - 1, 1)
    entries = jnp.clip(jax.random.normal(first_key, (TOKENS, D), jnp.float32), -3.0, 3.0)
    scales = 1.0 + 3.0 * share
    return jnp.clip(entries * scales[:, None], -18.0, 18.0).astype(jnp.bfloat16)


def draw_qkv_weight(key, part):
    first_key = jax.random.fold_in(key, 23)
    entries = jnp.clip(jax.random.normal(first_key, (D, (QH + 2 * KVH) * HD), jnp.float32), -6.0, 6.0) * D ** (-0.5)
    head_share = jnp.arange(KVH).astype(jnp.float32) / max(KVH - 1, 1)
    value_scales = 1.0 + 2.0 * head_share
    value_block = entries[:, (QH + KVH) * HD:].reshape(D, KVH, HD) * value_scales[None, :, None]
    entries = jnp.concatenate([entries[:, :(QH + KVH) * HD], value_block.reshape(D, KVH * HD)], axis=1)
    return jnp.clip(entries, -8.0, 8.0)


def levels(own_key, dims, cuts, low, high):
    def one(dim, parts):
        heights = jax.random.uniform(jax.random.fold_in(jax.random.fold_in(own_key, 6), dim), (parts,), jnp.float32, low / len(cuts), high / len(cuts))
        return jnp.repeat(jnp.exp(heights), dims[dim] // parts).reshape((-1,) + (1,) * (len(dims) - dim - 1))

    loudness = one(*cuts[0])
    for cut in cuts[1:]:
        loudness = loudness * one(*cut)
    return loudness


def length_profile(number_of, total, bound, skew):
    loads = [(1 << 20) // math.isqrt(rank ** skew) + 1 for rank in range(2, number_of + 1)]
    rest, given = total - bound - (number_of - 1), [1] * (number_of - 1)
    while rest > 0:
        movable = [i for i in range(number_of - 1) if given[i] < bound]
        whole, budget = sum([loads[i] for i in movable]), rest
        for i in movable:
            extra = min(bound - given[i], max(1, budget * loads[i] // whole), rest)
            given[i] = given[i] + extra
            rest = rest - extra
    return np.array([bound] + given)


def ragged(key, amount, total, bound, skew):
    if amount == 2:
        one = jax.random.randint(key, (), max(1, total - bound), min(bound, total - 1) + 1)
        return jnp.stack([one, total - one])
    lengths = jnp.asarray(length_profile(amount, total, bound, skew), jnp.int32)
    twos = (amount - 1) // 2
    source_of, receiver = lengths[1:1 + 2 * twos:2], lengths[2:2 + 2 * twos:2]
    room = jnp.minimum(source_of - 1, bound - receiver)
    moved = jax.random.randint(jax.random.fold_in(key, 1), (twos,), 0, 1 << 20) % (room + 1)
    lengths = lengths.at[1:1 + 2 * twos:2].set(source_of - moved).at[2:2 + 2 * twos:2].set(receiver + moved)
    return lengths[jax.random.permutation(jax.random.fold_in(key, 2), amount)]


def centred(own_key, shape, deviation, limit, shards=(), held_as=jnp.bfloat16):
    array = jax.random.normal(own_key, shape, jnp.float32) * deviation
    if len(shards) > 0:
        array = levels(own_key, shape, shards, -0.22, 0.18) * array
    return jnp.clip(array, min=-limit, max=limit).astype(held_as)


def setup_inputs(seed: int = 0) -> dict:
    streams_of = jax.random.split(jax.random.key(seed), 10)
    inputs = draw_inputs(jax.random.fold_in(streams_of[9], 71), 0)
    upstream = draw_upstream(jax.random.fold_in(streams_of[9], 71), 0)
    doc_ids = jnp.searchsorted(jnp.cumsum(ragged(streams_of[2], TOKENS // 48, TOKENS, 128, 1)), jnp.arange(TOKENS), side="right").astype(jnp.int32)
    qkv_weight = draw_qkv_weight(jax.random.fold_in(streams_of[9], 71), 0)
    out_weight = centred(streams_of[4], (D, D), D ** -0.5, 0.125, ((0, 128),), jnp.float32)
    qkv_mean = centred(streams_of[5], (D, QKV_COLS), 0.5, 3.0, ((0, 128),), jnp.float32)
    qkv_square = jnp.clip(jnp.exp(math.log(3.0) - 2.3025851 * jax.random.uniform(streams_of[6], (D, QKV_COLS), jnp.float32) ** levels(streams_of[6], (D, QKV_COLS), ((0, 128),), -0.2, 0.2)), 0.3, 3.0)
    out_mean = centred(streams_of[7], (D, D), 0.5, 3.0, ((0, 128),), jnp.float32)
    out_square = jnp.clip(jnp.exp(math.log(3.0) - 2.3025851 * jax.random.uniform(streams_of[8], (D, D), jnp.float32) ** levels(streams_of[8], (D, D), ((0, 128),), -0.2, 0.2)), 0.3, 3.0)
    return dict(inputs=inputs, upstream=upstream, doc_ids=doc_ids, qkv_weight=qkv_weight, out_weight=out_weight, qkv_mean=qkv_mean, qkv_square=qkv_square, out_mean=out_mean, out_square=out_square)


beta_one = 0.9
beta_two = 0.95
learn_rate = 0.0003
decay_rate = 0.1
epsilon = 1e-08
step_count = 10
norm_eps = 1e-05
masked_score = -1e+30

def normalize(rows_in):
    values = rows_in.astype(jnp.float32)
    factor = lax.rsqrt(lax.optimization_barrier(jnp.mean(values * values, axis=-1, keepdims=True)) + norm_eps)
    return (values * factor).astype(jnp.bfloat16)

def split_heads(qkv_rows):
    length = qkv_rows.shape[0]
    query_part = qkv_rows[:, :QH * HD].reshape(length, KVH, QH // KVH, HD)
    key_part = qkv_rows[:, QH * HD:(QH + KVH) * HD].reshape(length, KVH, HD)
    value_part = qkv_rows[:, (QH + KVH) * HD:].reshape(length, KVH, HD)
    return (query_part.astype(jnp.float32), key_part.astype(jnp.float32), value_part.astype(jnp.float32))

def device_pass(rows_in, upstream_rows, doc_rows, qkv_b, out_b):
    length = rows_in.shape[0]
    score_scale = HD ** (-0.5)
    normed = normalize(rows_in)
    qkv_rows = jnp.dot(normed, qkv_b, preferred_element_type=jnp.float32).astype(jnp.bfloat16)
    query_part, key_part, value_part = split_heads(qkv_rows)
    scores = jnp.einsum('tkgd,skd->kgts', query_part, key_part) * score_scale
    position = jnp.arange(length)
    allowed = (position[:, None] >= position[None, :]) & (doc_rows[:, None] == doc_rows[None, :])
    scores = jnp.where(allowed, scores, masked_score)
    row_max = lax.optimization_barrier(jnp.max(scores, axis=-1, keepdims=True))
    exponent = jnp.exp(scores - row_max)
    soft = exponent / lax.optimization_barrier(jnp.sum(exponent, axis=-1, keepdims=True))
    soft_b = soft.astype(jnp.bfloat16)
    soft_wide = soft_b.astype(jnp.float32)
    mixed_rows = jnp.einsum('kgts,skd->tkgd', soft_wide, value_part).astype(jnp.bfloat16).reshape(length, QH * HD)
    attn_rows = jnp.dot(mixed_rows, out_b, preferred_element_type=jnp.float32).astype(jnp.bfloat16)
    d_mixed = jnp.dot(upstream_rows, out_b.T, preferred_element_type=jnp.float32).astype(jnp.bfloat16)
    d_heads = d_mixed.reshape(length, KVH, QH // KVH, HD).astype(jnp.float32)
    d_value = jnp.einsum('kgts,tkgd->skd', soft_wide, d_heads).astype(jnp.bfloat16)
    d_soft = jnp.einsum('tkgd,skd->kgts', d_heads, value_part)
    row_delta = lax.optimization_barrier(jnp.sum(soft * d_soft, axis=-1, keepdims=True))
    d_scores = (soft * (d_soft - row_delta)).astype(jnp.bfloat16).astype(jnp.float32)
    d_query = (jnp.einsum('kgts,skd->tkgd', d_scores, key_part) * score_scale).astype(jnp.bfloat16)
    d_key = (jnp.einsum('kgts,tkgd->skd', d_scores, query_part) * score_scale).astype(jnp.bfloat16)
    d_qkv = jnp.concatenate([d_query.reshape(length, QH * HD), d_key.reshape(length, KVH * HD), d_value.reshape(length, KVH * HD)], axis=1)
    grad_qkv = jnp.dot(normed.T, d_qkv, preferred_element_type=jnp.float32)
    grad_out = jnp.dot(mixed_rows.T, upstream_rows, preferred_element_type=jnp.float32)
    term = jnp.concatenate([grad_qkv, grad_out], axis=1).astype(jnp.bfloat16)
    return (attn_rows, term)

def adamw(weight, mean_in, square_in, grad):
    new_mean = beta_one * mean_in + (1.0 - beta_one) * grad
    new_square = beta_two * square_in + (1.0 - beta_two) * grad * grad
    corrected = new_mean / (1.0 - beta_one ** step_count) / (jnp.sqrt(new_square / (1.0 - beta_two ** step_count)) + epsilon)
    return (weight - learn_rate * (corrected + decay_rate * weight), new_mean, new_square)

def reference(inputs, upstream, doc_ids, qkv_weight, out_weight, qkv_mean, qkv_square, out_mean, out_square):
    qkv_b = qkv_weight.astype(jnp.bfloat16)
    out_b = out_weight.astype(jnp.bfloat16)
    qkv_cols = qkv_weight.shape[1]
    split_in = inputs.reshape(N_GRP, N_DP, TOK_DEV, D)
    split_up = upstream.reshape(N_GRP, N_DP, TOK_DEV, D)
    split_docs = doc_ids.reshape(N_GRP, N_DP, TOK_DEV)

    def one_group(packed):
        group_in, group_up, group_docs = packed

        def one_device(running, device):
            attn_rows, term = device_pass(device[0], device[1], device[2], qkv_b, out_b)
            term = lax.optimization_barrier(term)
            return (running + term.astype(jnp.float32), attn_rows)
        start_sum = jnp.zeros((D, qkv_cols + D), jnp.float32)
        running, attn_rows = lax.scan(one_device, start_sum, (group_in, group_up, group_docs))
        return (running.astype(jnp.bfloat16), attn_rows)
    group_sums, attn_all = lax.map(one_group, (split_in, split_up, split_docs))
    group_sums = lax.optimization_barrier(group_sums)
    gradient = lax.optimization_barrier(jnp.sum(group_sums.astype(jnp.float32), axis=0))
    squares = jnp.sum(gradient * gradient)
    param_count = D * (qkv_cols + D)
    clip = jnp.minimum(1.0, jnp.sqrt(jnp.float32(param_count)) / (jnp.sqrt(squares) + 1e-06))
    clipped = clip * gradient
    new_qkv_weight, new_qkv_mean, new_qkv_square = adamw(qkv_weight, qkv_mean, qkv_square, clipped[:, :qkv_cols])
    new_out_weight, new_out_mean, new_out_square = adamw(out_weight, out_mean, out_square, clipped[:, qkv_cols:])
    attn_out = attn_all.reshape(TOKENS, D)
    return (attn_out, new_qkv_weight, new_out_weight, new_qkv_mean, new_qkv_square, new_out_mean, new_out_square)
```

```python
import math

import jax
import jax.numpy as jnp
import numpy as np
from jax import lax
from jax.experimental import pallas as pl
from jax.experimental.pallas import tpu as pltpu
from jax.sharding import Mesh
from jax.sharding import PartitionSpec as P

HD = 128
TOK = 384
ALL = ("grp", "dp_0", "dp_1", "dp_2")

beta_one = 0.9
beta_two = 0.95
learn_rate = 0.0003
decay_rate = 0.1
epsilon = 1e-08
step_count = 10
norm_eps = 1e-05
masked_score = -1e30
scale = HD ** (-0.5)


MASKS = [(1 if d % 2 == 0 else 3) << (2 * (2 - d // 2)) for d in range(6)]
LATE = ((0, 2, 4), (1, 3, 5))
EARLY = ((1, 3, 5), (0, 2, 4))


def late_links(rotation, stage):
    return tuple(LATE[c][(rotation + stage) % 3] for c in range(2))


def early_links(stage):
    return tuple(EARLY[c][stage] for c in range(2))


def block_masks():
    table = np.zeros((2, 3, 64), np.int32)
    for c in range(2):
        for rotation in range(3):
            for p in range(64):
                m = 0
                for bit in range(3):
                    if p >> bit & 1:
                        m ^= MASKS[EARLY[c][bit]]
                    if p >> (3 + bit) & 1:
                        m ^= MASKS[LATE[c][(rotation + bit) % 3]]
                table[c, rotation, p] = m
    return table


TABLE = block_masks()


def across(x, links):
    pairs = [((t * 2 + c), ((t ^ MASKS[links[c]]) * 2 + c)) for t in range(64) for c in range(2)]
    return lax.ppermute(x, ALL, pairs)


def to_partner(x):
    return lax.ppermute(x, "dp_2", [(0, 1), (1, 0)])


def out_pairs():
    pairs = []
    for chip in range(64):
        for c in range(2):
            x = chip >> 4
            target = ((x % 2) * 2 + c) * 16 + (chip & 15)
            pairs.append((chip * 2 + c, target * 2 + x // 2))
    return pairs


def out_row(t):
    xp = t >> 4
    return ((xp >> 1) * 16 + (t & 15)) * 2 + (xp & 1)


def normalize(rows_in):
    values = rows_in.astype(jnp.float32)
    factor = lax.rsqrt(jnp.mean(values * values, axis=-1, keepdims=True) + norm_eps)
    return (values * factor).astype(jnp.bfloat16)


ANY = pl.BlockSpec(memory_space=pl.ANY)
SMEM = pl.BlockSpec(memory_space=pltpu.SMEM)
VMEM = pl.BlockSpec(memory_space=pltpu.VMEM)
BF = jnp.bfloat16
F32 = jnp.float32


def cost(flops, nbytes):
    return pl.CostEstimate(flops=flops, bytes_accessed=nbytes, transcendentals=0)


def project_body(ids, x_ref, a_ref, b_ref, o_ref, w, sem):
    def step(p, carry):
        pltpu.make_async_copy(a_ref.at[p], w.at[ids[p]], sem).start()
        pltpu.make_async_copy(b_ref.at[p], w.at[ids[p + 32]], sem).start()
        return carry

    lax.fori_loop(0, 32, step, 0)
    pltpu.make_async_copy(w, w, sem).wait()
    o_ref[...] = jnp.dot(
        x_ref[...], w[...].reshape(2048, 512), preferred_element_type=F32
    ).astype(BF)


def project(ids, x, a, b):
    return pl.pallas_call(
        project_body,
        in_specs=[SMEM, VMEM, ANY, ANY],
        out_specs=VMEM,
        out_shape=jax.ShapeDtypeStruct((2 * TOK, 512), BF),
        scratch_shapes=[pltpu.VMEM((64, 32, 512), BF), pltpu.SemaphoreType.DMA],
        cost_estimate=cost(2 * 768 * 2048 * 512, 8 << 20),
        name="project",
    )(ids, x, a, b)


def d_mixed_body(ids3, ids4, u_ref, a3, b3, a4, b4, o_ref, w_ref, sem):
    def step(p, carry):
        for ids, a, b, first in ((ids3, a3, b3, 0), (ids4, a4, b4, 2)):
            for part in range(2):
                cols = pl.ds(512 * (first + part), 512)
                rows = pl.ds(16 * part, 16)
                pltpu.make_async_copy(
                    a.at[p, rows, :], w_ref.at[out_row(ids[p]), :, cols], sem
                ).start()
                pltpu.make_async_copy(
                    b.at[p, rows, :], w_ref.at[out_row(ids[p + 32]), :, cols], sem
                ).start()
        return carry

    lax.fori_loop(0, 32, step, 0)
    pltpu.make_async_copy(w_ref, w_ref, sem).wait()
    o_ref[...] = lax.dot_general(
        u_ref[...],
        w_ref[...].reshape(1024, 2048),
        (((1,), (1,)), ((), ())),
        preferred_element_type=F32,
    ).astype(BF)


def d_mixed_call(ids3, ids4, u, a3, b3, a4, b4):
    return pl.pallas_call(
        d_mixed_body,
        in_specs=[SMEM, SMEM, VMEM, ANY, ANY, ANY, ANY],
        out_specs=(VMEM, VMEM),
        out_shape=(
            jax.ShapeDtypeStruct((2 * TOK, 1024), BF),
            jax.ShapeDtypeStruct((64, 16, 2048), BF),
        ),
        scratch_shapes=[pltpu.SemaphoreType.DMA],
        cost_estimate=cost(2 * 768 * 2048 * 1024, 12 << 20),
        name="d_mixed",
    )(ids3, ids4, u, a3, b3, a4, b4)


def stacked(ref, rows):
    return jnp.concatenate([ref[rows, HD * h : HD * (h + 1)] for h in range(4)], axis=0)


def nt(a, b):
    return lax.dot_general(a, b, (((1,), (1,)), ((), ())), preferred_element_type=F32)


def tn(a, b):
    return lax.dot_general(a, b, (((0,), (0,)), ((), ())), preferred_element_type=F32)


def softmax_block(q_ref, k_ref, col_ref, row_ref, i):
    lo, hi = max(0, 128 * (i - 1)), 128 * (i + 1)
    n = hi - lo
    rows = slice(128 * i, 128 * (i + 1))
    q = stacked(q_ref, rows)
    scores = nt(q, k_ref[lo:hi, :]) * scale
    t = lax.broadcasted_iota(jnp.int32, (128, n), 0) + 128 * i
    s = lax.broadcasted_iota(jnp.int32, (128, n), 1) + lo
    allowed = (t >= s) & (col_ref[rows, :] == row_ref[0, :, lo:hi])
    scores = jnp.where(allowed[None], scores.reshape(4, 128, n), masked_score).reshape(512, n)
    exponent = jnp.exp(scores - jnp.max(scores, axis=-1, keepdims=True))
    soft = exponent * (1.0 / jnp.sum(exponent, axis=-1, keepdims=True))
    return q, soft, rows, lo, hi


def forward_body(q_ref, k_ref, v_ref, col_ref, row_ref, o_ref):
    for i in range(3):
        q, soft, rows, lo, hi = softmax_block(q_ref, k_ref, col_ref, row_ref, i)
        mixed = jnp.dot(soft.astype(BF), v_ref[lo:hi, :], preferred_element_type=F32).astype(BF)
        for h in range(4):
            o_ref[rows, HD * h : HD * (h + 1)] = mixed[128 * h : 128 * (h + 1)]


def attention_specs(g):
    return [
        pl.BlockSpec((TOK, 512), lambda s: (s, 0)),
        pl.BlockSpec((TOK, HD), lambda s, g=g: (s, g)),
        pl.BlockSpec((TOK, HD), lambda s, g=g: (s, 2 + g)),
        pl.BlockSpec((TOK, 1), lambda s: (s, 0)),
        pl.BlockSpec((1, 1, TOK), lambda s: (s, 0, 0)),
    ]


def forward(g, q, kv, col, row):
    return pl.pallas_call(
        forward_body,
        grid=(2,),
        in_specs=attention_specs(g),
        out_specs=pl.BlockSpec((TOK, 512), lambda s: (s, 0)),
        out_shape=jax.ShapeDtypeStruct((2 * TOK, 512), BF),
        cost_estimate=cost(2 * 2 * 512 * 640 * 128 * 6, 3 << 20),
        name="attend",
    )(q, kv, kv, col, row)


def backward_body(q_ref, k_ref, v_ref, col_ref, row_ref, d_ref, dq_ref, dk_ref, dv_ref, dk, dv):
    dk[...] = jnp.zeros_like(dk)
    dv[...] = jnp.zeros_like(dv)
    for i in range(3):
        q, soft, rows, lo, hi = softmax_block(q_ref, k_ref, col_ref, row_ref, i)
        d_heads = stacked(d_ref, rows)
        d_soft = nt(d_heads, v_ref[lo:hi, :])
        delta = jnp.sum(soft * d_soft, axis=-1, keepdims=True)
        d_scores = (soft * (d_soft - delta)).astype(BF)
        dv[lo:hi, :] += tn(soft.astype(BF), d_heads)
        dk[lo:hi, :] += tn(d_scores, q)
        d_query = (
            jnp.dot(d_scores, k_ref[lo:hi, :], preferred_element_type=F32) * scale
        ).astype(BF)
        for h in range(4):
            dq_ref[rows, HD * h : HD * (h + 1)] = d_query[128 * h : 128 * (h + 1)]
    dk_ref[...] = (dk[...] * scale).astype(BF)
    dv_ref[...] = dv[...].astype(BF)


def backward(g, q, kv, col, row, d_mixed):
    return pl.pallas_call(
        backward_body,
        grid=(2,),
        in_specs=attention_specs(g) + [pl.BlockSpec((TOK, 512), lambda s, g=g: (s, g))],
        out_specs=(
            pl.BlockSpec((TOK, 512), lambda s: (s, 0)),
            pl.BlockSpec((TOK, HD), lambda s: (s, 0)),
            pl.BlockSpec((TOK, HD), lambda s: (s, 0)),
        ),
        out_shape=(
            jax.ShapeDtypeStruct((2 * TOK, 512), BF),
            jax.ShapeDtypeStruct((2 * TOK, HD), BF),
            jax.ShapeDtypeStruct((2 * TOK, HD), BF),
        ),
        scratch_shapes=[pltpu.VMEM((TOK, HD), F32), pltpu.VMEM((TOK, HD), F32)],
        cost_estimate=cost(2 * 2 * 512 * 640 * 128 * 15, 5 << 20),
        name="attend_back",
    )(q, kv, kv, col, row, d_mixed)


HALF = jax.ShapeDtypeStruct((32, 32, 512), BF)


def grad_out_body(ids, m0_ref, m1_ref, u_ref, keep, send, g, sem):
    g[0:32] = tn(m0_ref[...], u_ref[...]).astype(BF).reshape(32, 16, 1024)
    g[32:64] = tn(m1_ref[...], u_ref[...]).astype(BF).reshape(32, 16, 1024)

    def step(p, carry):
        for part in range(2):
            cols = pl.ds(512 * part, 512)
            rows = pl.ds(16 * part, 16)
            pltpu.make_async_copy(
                g.at[out_row(ids[p]), :, cols], keep.at[p, rows, :], sem
            ).start()
            pltpu.make_async_copy(
                g.at[out_row(ids[p + 32]), :, cols], send.at[p, rows, :], sem
            ).start()
        return carry

    lax.fori_loop(0, 32, step, 0)
    pltpu.make_async_copy(g, g, sem).wait()


def grad_out_call(ids, m0, m1, u, half):
    return pl.pallas_call(
        grad_out_body,
        grid=(1,),
        in_specs=[
            SMEM,
            pl.BlockSpec((2 * TOK, 512), lambda i: (0, 0)),
            pl.BlockSpec((2 * TOK, 512), lambda i: (0, 0)),
            pl.BlockSpec((2 * TOK, 1024), lambda i: (0, half)),
        ],
        out_specs=(ANY, ANY),
        out_shape=(HALF, HALF),
        scratch_shapes=[pltpu.VMEM((64, 16, 1024), BF), pltpu.SemaphoreType.DMA],
        cost_estimate=cost(2 * 768 * 1024 * 1024, 5 << 20),
        name="grad_out",
    )(ids, m0, m1, u)


def grad_qkv_body(ids, x_ref, *refs):
    d_refs, (keep, send, g, sem) = refs[:-4], refs[-4:]
    if len(d_refs) == 1:
        d = d_refs[0][...]
    else:
        d = jnp.concatenate([r[...] for r in d_refs], axis=1)
    g[...] = tn(x_ref[...], d).astype(BF).reshape(64, 32, 512)

    def step(p, carry):
        pltpu.make_async_copy(g.at[ids[p]], keep.at[p], sem).start()
        pltpu.make_async_copy(g.at[ids[p + 32]], send.at[p], sem).start()
        return carry

    lax.fori_loop(0, 32, step, 0)
    pltpu.make_async_copy(g, g, sem).wait()


def grad_qkv_call(ids, x, *d):
    return pl.pallas_call(
        grad_qkv_body,
        in_specs=[SMEM, VMEM] + [VMEM] * len(d),
        out_specs=(ANY, ANY),
        out_shape=(HALF, HALF),
        scratch_shapes=[pltpu.VMEM((64, 32, 512), BF), pltpu.SemaphoreType.DMA],
        cost_estimate=cost(2 * 768 * 2048 * 512, 6 << 20),
        name="grad_qkv",
    )(ids, x, *d)


def added(a, b):
    return (a.astype(F32) + b.astype(F32)).astype(BF)


def late_reduce(keep, send, rotation):
    for stage in (2, 1, 0):
        recv = across(send, late_links(rotation, stage))
        n = keep.shape[0] // 2
        if stage == 0:
            return added(keep, recv)
        send = added(keep[n:], recv[n:])
        keep = added(keep[:n], recv[:n])


def early_reduce(x):
    for stage in (2, 1, 0):
        n = x.shape[0] // 2
        recv = across(x[n:], early_links(stage))
        if stage == 0:
            return x[0].astype(F32) + recv[0].astype(F32)
        x = added(x[:n], recv)


def adamw(weight, mean_in, square_in, grad):
    new_mean = beta_one * mean_in + (1.0 - beta_one) * grad
    new_square = beta_two * square_in + (1.0 - beta_two) * grad * grad
    corrected = (
        new_mean
        / (1.0 - beta_one**step_count)
        / (jnp.sqrt(new_square / (1.0 - beta_two**step_count)) + epsilon)
    )
    return (weight - learn_rate * (corrected + decay_rate * weight), new_mean, new_square)


def halves(rows):
    return [
        jnp.concatenate(
            [
                rows[:, 1024 * h : 1024 * (h + 1)],
                rows[:, 2048 + 256 * h : 2048 + 256 * (h + 1)],
                rows[:, 2560 + 256 * h : 2560 + 256 * (h + 1)],
            ],
            axis=1,
        )
        for h in range(2)
    ]


def local(
    inputs, upstream, doc_ids, qkv_weight, out_weight, qkv_mean, qkv_square, out_mean, out_square
):
    core = lax.axis_index("dp_2")
    chip = lax.axis_index(("grp", "dp_0", "dp_1"))
    first = core == 0
    ids = jnp.where(first, TABLE[0], TABLE[1]) ^ chip
    rot = (0, 1, 2, 0, 1)

    out_block = lax.ppermute(out_weight.astype(BF), ALL, out_pairs())
    h0, h1 = halves(qkv_weight.astype(BF))
    mine, theirs = jnp.where(first, h0, h1), jnp.where(first, h1, h0)
    arrived = to_partner(theirs)
    top, bottom = jnp.where(first, mine, arrived), jnp.where(first, arrived, mine)
    block = jnp.concatenate(
        [
            part[:, 512 * s : 512 * (s + 1)]
            for s in range(3)
            for part in (top, bottom)
        ]
        + [out_block[:, 512 * s : 512 * (s + 1)] for s in range(4)],
        axis=0,
    )[None]
    for stage in range(3):
        block = jnp.concatenate([block, across(block, early_links(stage))], axis=0)
    streams = []
    for s in range(5):
        have = block[:, 32 * s : 32 * (s + 1), :]
        for stage in range(2):
            have = jnp.concatenate([have, across(have, late_links(rot[s], stage))], axis=0)
        streams.append((have, across(have, late_links(rot[s], 2))))

    both = jnp.concatenate([inputs, to_partner(inputs)], axis=0)
    up = jnp.concatenate([upstream, to_partner(upstream)], axis=0)
    docs = jnp.stack([doc_ids, to_partner(doc_ids)])
    col, row = docs.reshape(2 * TOK, 1), docs.reshape(2, 1, TOK)
    normed = normalize(both)

    q0, q1, kv = (project(ids[rot[s]], normed, *streams[s]) for s in range(3))
    m0 = forward(0, q0, kv, col, row)
    m1 = forward(1, q1, kv, col, row)
    d_mixed, out_half = d_mixed_call(ids[rot[3]], ids[rot[4]], up, *streams[3], *streams[4])
    partial = []
    for h in range(2):
        keep, send = grad_out_call(ids[rot[3 + h]], m0, m1, up, h)
        partial.append(late_reduce(keep, send, rot[3 + h]))
    out_sum = early_reduce(jnp.concatenate(partial, axis=1))

    dq0, dk0, dv0 = backward(0, q0, kv, col, row, d_mixed)
    keep0 = late_reduce(*grad_qkv_call(ids[rot[0]], normed, dq0), rot[0])
    dq1, dk1, dv1 = backward(1, q1, kv, col, row, d_mixed)
    keep1 = late_reduce(*grad_qkv_call(ids[rot[1]], normed, dq1), rot[1])
    keep2 = late_reduce(*grad_qkv_call(ids[rot[2]], normed, dk0, dk1, dv0, dv1), rot[2])
    qkv_sum = early_reduce(jnp.concatenate([keep0, keep1, keep2], axis=1))

    out_half = out_half.reshape(1024, 2048)
    mixed = jnp.concatenate([m0, m1], axis=1)
    other = jnp.dot(mixed[TOK:], out_half, preferred_element_type=F32)
    own = jnp.dot(mixed[:TOK], out_half, preferred_element_type=F32)
    attn_out = (own + to_partner(other)).astype(BF)

    squares = jnp.sum(qkv_sum * qkv_sum) + jnp.sum(out_sum * out_sum)
    spread = lax.all_to_all(
        jnp.full((128, 128), squares, F32), ALL, split_axis=0, concat_axis=0, tiled=True
    )
    squares = jnp.sum(spread[:, 0])
    rows = qkv_sum.reshape(3, 2, 16, 512)
    mine = jnp.where(first, rows[:, 0], rows[:, 1])
    arrived = to_partner(jnp.where(first, rows[:, 1], rows[:, 0]))
    low, high = jnp.where(first, mine, arrived), jnp.where(first, arrived, mine)
    grad_qkv = jnp.concatenate(
        [low[0], low[1], high[0], high[1]]
        + [low[2, :, :256], high[2, :, :256], low[2, :, 256:], high[2, :, 256:]],
        axis=1,
    )
    back = [(b, a) for a, b in out_pairs()]
    out_rows = jnp.concatenate([out_sum[16 * s : 16 * (s + 1)] for s in range(4)], axis=1)
    grad_out = lax.ppermute(out_rows, ALL, back)

    param_count = 2048 * (3072 + 2048)
    clip = jnp.minimum(1.0, math.sqrt(param_count) / (jnp.sqrt(squares) + 1e-06))
    new_qkv_weight, new_qkv_mean, new_qkv_square = adamw(
        qkv_weight, qkv_mean, qkv_square, clip * grad_qkv
    )
    new_out_weight, new_out_mean, new_out_square = adamw(
        out_weight, out_mean, out_square, clip * grad_out
    )
    return (
        attn_out,
        new_qkv_weight,
        new_out_weight,
        new_qkv_mean,
        new_qkv_square,
        new_out_mean,
        new_out_square,
    )


def solution(mesh):
    finer = Mesh(mesh.devices.reshape(4, 4, 4, 2), ALL)
    wide = P(ALL, None)
    return jax.shard_map(
        local,
        mesh=finer,
        in_specs=(wide, wide, P(ALL), wide, wide, wide, wide, wide, wide),
        out_specs=(wide,) * 7,
        check_vma=False,
    )
```

```python
import math

import jax
import jax.numpy as jnp
import numpy as np
from jax import lax
from jax.experimental import pallas as pl
from jax.experimental.pallas import tpu as pltpu
from jax.sharding import Mesh
from jax.sharding import PartitionSpec as P


HD = 128
TOK = 384
ALL = ("grp", "dp_0", "dp_1", "dp_2")

beta_one = 0.9
beta_two = 0.95
learn_rate = 0.0003
decay_rate = 0.1
epsilon = 1e-08
step_count = 10
norm_eps = 1e-05
masked_score = -1e30
scale = HD ** (-0.5)


MASKS = [(1 if d % 2 == 0 else 3) << (2 * (2 - d // 2)) for d in range(6)]
LATE = ((0, 2, 4), (1, 3, 5))
EARLY = ((1, 3, 5), (0, 2, 4))


def late_links(rotation, stage):
    return tuple(MASKS[LATE[c][(rotation + stage) % 3]] for c in range(2))


def early_mask(core, p):
    m = 0
    for bit in range(3):
        if p >> bit & 1:
            m ^= MASKS[EARLY[core][bit]]
    return m


def block_masks():
    table = np.zeros((2, 3, 64), np.int32)
    for c in range(2):
        for rotation in range(3):
            for p in range(64):
                m = early_mask(c, p)
                for bit in range(3):
                    if p >> (3 + bit) & 1:
                        m ^= MASKS[LATE[c][(rotation + bit) % 3]]
                table[c, rotation, p] = m
    return table


TABLE = block_masks()


def across(x, masks):
    pairs = [((t * 2 + c), ((t ^ masks[c]) * 2 + c)) for t in range(64) for c in range(2)]
    return lax.ppermute(x, ALL, pairs)


def early(x, p):
    return across(x, [early_mask(c, p) for c in range(2)])


def to_partner(x):
    return lax.ppermute(x, "dp_2", [(0, 1), (1, 0)])


def out_pairs():
    pairs = []
    for chip in range(64):
        for c in range(2):
            x = chip >> 4
            target = ((x % 2) * 2 + c) * 16 + (chip & 15)
            pairs.append((chip * 2 + c, target * 2 + x // 2))
    return pairs


def out_row(t):
    xp = t >> 4
    return ((xp >> 1) * 16 + (t & 15)) * 2 + (xp & 1)


def normalize(rows_in):
    values = rows_in.astype(jnp.float32)
    factor = lax.rsqrt(jnp.mean(values * values, axis=-1, keepdims=True) + norm_eps)
    return (values * factor).astype(jnp.bfloat16)


ANY = pl.BlockSpec(memory_space=pl.ANY)
SMEM = pl.BlockSpec(memory_space=pltpu.SMEM)
VMEM = pl.BlockSpec(memory_space=pltpu.VMEM)
BF = jnp.bfloat16
F32 = jnp.float32


def cost(flops, nbytes):
    return pl.CostEstimate(flops=flops, bytes_accessed=nbytes, transcendentals=0)


def place_stream(ids, rotation, a, b, w, sem):
    def step(p, carry):
        pltpu.make_async_copy(a.at[p], w.at[ids[rotation, p]], sem).start()
        pltpu.make_async_copy(b.at[p], w.at[ids[rotation, p + 32]], sem).start()
        return carry

    lax.fori_loop(0, 32, step, 0, unroll=4)


def nn(a, b):
    return jnp.dot(a, b, preferred_element_type=F32)


def nt(a, b):
    return lax.dot_general(a, b, (((1,), (1,)), ((), ())), preferred_element_type=F32)


def tn(a, b):
    return lax.dot_general(a, b, (((0,), (0,)), ((), ())), preferred_element_type=F32)


def stacked(ref, g, rows):
    return jnp.concatenate([ref[g, rows, HD * h : HD * (h + 1)] for h in range(4)], axis=0)


def softmax_block(q_ref, kv_ref, col_ref, row_ref, g, seq, i):
    lo, hi = max(0, 128 * (i - 1)), 128 * (i + 1)
    n = hi - lo
    base = seq * TOK
    rows = pl.ds(pl.multiple_of(base + 128 * i, 128), 128)
    keys = pl.ds(pl.multiple_of(base + lo, 128), n)
    q = stacked(q_ref, g, rows)
    scores = nt(q, kv_ref[g, keys, :]) * scale
    t = lax.broadcasted_iota(jnp.int32, (128, n), 0) + 128 * i
    s = lax.broadcasted_iota(jnp.int32, (128, n), 1) + lo
    allowed = (t >= s) & (col_ref[rows, :] == row_ref[seq, :, lo:hi])
    scores = jnp.where(allowed[None], scores.reshape(4, 128, n), masked_score).reshape(512, n)
    exponent = jnp.exp(scores - jnp.max(scores, axis=-1, keepdims=True))
    soft = exponent * (1.0 / jnp.sum(exponent, axis=-1, keepdims=True))
    return q, soft, rows, keys


def load_rows(own, other, dst, sem):
    pltpu.make_async_copy(own, dst.at[pl.ds(0, TOK)], sem).start()
    pltpu.make_async_copy(other, dst.at[pl.ds(TOK, TOK)], sem).start()


def wait_all(ref, sem):
    pltpu.make_async_copy(ref, ref, sem).wait()


def spread_out_rows(ids, half, g, keep, send, sem):
    def step(p, carry):
        for part in range(2):
            cols = pl.ds(512 * part, 512)
            rows = pl.ds(16 * part, 16)
            pltpu.make_async_copy(
                g.at[half, out_row(ids[half, p + 32]), :, cols], send.at[p, rows, :], sem
            ).start()
            pltpu.make_async_copy(
                g.at[half, out_row(ids[half, p]), :, cols], keep.at[p, rows, :], sem
            ).start()
        return carry

    lax.fori_loop(0, 32, step, 0)


def project_body(*refs):
    ids, xa, xb, ua, ub, a0, b0, a1, b1, a2, b2, col_ref, row_ref = refs[:13]
    q_ref, kv_ref, o_ref, keep3, send3, keep4, send4 = refs[13:20]
    x, u, w, rows_out, g, sems = refs[20:]
    pairs = ((a0, b0), (a1, b1), (a2, b2))
    load_rows(xa, xb, x, sems.at[3])
    for s in range(3):
        place_stream(ids, s, *pairs[s], w.at[s], sems.at[s])
    load_rows(ua, ub, u, sems.at[4])
    wait_all(x, sems.at[3])

    def column(s, carry):
        wait_all(w.at[s], sems.at[s])
        rows_out[s] = nn(x[...], w[s].reshape(2048, 512)).astype(BF)
        return carry

    lax.fori_loop(0, 3, column, 0)
    q_ref[...] = rows_out[0:2]
    for j in range(4):
        kv_ref[j] = rows_out[2, :, HD * j : HD * (j + 1)]

    def unit(n, carry):
        h, seq = n // 2, n % 2
        for i in range(3):
            _, soft, rows, keys = softmax_block(q_ref, kv_ref, col_ref, row_ref, h, seq, i)
            mixed = nn(soft.astype(BF), kv_ref[2 + h, keys, :]).astype(BF)
            for j in range(4):
                o_ref[h, rows, HD * j : HD * (j + 1)] = mixed[128 * j : 128 * (j + 1)]
        return carry

    lax.fori_loop(0, 4, unit, 0)
    wait_all(u, sems.at[4])
    for half, keep, send in ((0, keep3, send3), (1, keep4, send4)):

        def group(h, carry):
            out = tn(o_ref[h], u[:, 1024 * half : 1024 * (half + 1)]).astype(BF)
            g[half, pl.ds(32 * h, 32)] = out.reshape(32, 16, 1024)
            return carry

        lax.fori_loop(0, 2, group, 0)
        spread_out_rows(ids, half, g, keep, send, sems.at[5 + half])
    for half in range(2):
        wait_all(g.at[half], sems.at[5 + half])


PAIR = jax.ShapeDtypeStruct((2, 2 * TOK, 512), BF)
HALF = jax.ShapeDtypeStruct((32, 32, 512), BF)


ROWS = pltpu.VMEM((2 * TOK, 2048), BF)


def project(ids, x, u, streams, col, row):
    return pl.pallas_call(
        project_body,
        in_specs=[SMEM] + [ANY] * 10 + [VMEM] * 2,
        out_specs=(VMEM,) * 3 + (ANY,) * 4,
        out_shape=(PAIR, jax.ShapeDtypeStruct((4, 2 * TOK, HD), BF), PAIR) + (HALF,) * 4,
        scratch_shapes=[
            ROWS,
            ROWS,
            pltpu.VMEM((3, 64, 32, 512), BF),
            pltpu.VMEM((3, 2 * TOK, 512), BF),
            pltpu.VMEM((2, 64, 16, 1024), BF),
            pltpu.SemaphoreType.DMA((7,)),
        ],
        cost_estimate=cost(2 * 768 * 2048 * 2560, 20 << 20),
        name="project",
    )(ids, *x, *u, *[piece for pair in streams for piece in pair], col, row)


def backward_body(*refs):
    ids, xa, xb, ua, ub, a3, b3, a4, b4, q_ref, kv_ref, col_ref, row_ref = refs[:13]
    w_ref, keep0, send0, keep1, send1, keep2, send2 = refs[13:20]
    x, u, d_ref, dq, dkv, g, acc, sems = refs[20:]
    load_rows(ua, ub, u, sems.at[0])

    def place(p, carry):
        for r, a, b, first in ((0, a3, b3, 0), (1, a4, b4, 2)):
            for part in range(2):
                cols = pl.ds(512 * (first + part), 512)
                rows = pl.ds(16 * part, 16)
                pltpu.make_async_copy(
                    a.at[p, rows, :], w_ref.at[out_row(ids[r, p]), :, cols], sems.at[1]
                ).start()
                pltpu.make_async_copy(
                    b.at[p, rows, :], w_ref.at[out_row(ids[r, p + 32]), :, cols], sems.at[1]
                ).start()
        return carry

    lax.fori_loop(0, 32, place, 0)
    load_rows(xa, xb, x, sems.at[2])
    wait_all(u, sems.at[0])
    wait_all(w_ref, sems.at[1])

    def heads(h, carry):
        d_ref[h] = nt(u[...], w_ref[pl.ds(32 * h, 32)].reshape(512, 2048)).astype(BF)
        return carry

    lax.fori_loop(0, 2, heads, 0)

    def unit(n, carry):
        h, seq = n // 2, n % 2
        acc[...] = jnp.zeros_like(acc)
        for i in range(3):
            q, soft, rows, keys = softmax_block(q_ref, kv_ref, col_ref, row_ref, h, seq, i)
            own = slice(max(0, 128 * (i - 1)), 128 * (i + 1))
            d_heads = stacked(d_ref, h, rows)
            d_soft = nt(d_heads, kv_ref[2 + h, keys, :])
            delta = jnp.sum(soft * d_soft, axis=-1, keepdims=True)
            d_scores = (soft * (d_soft - delta)).astype(BF)
            acc[1, own, :] += tn(soft.astype(BF), d_heads)
            acc[0, own, :] += tn(d_scores, q)
            d_query = (nn(d_scores, kv_ref[h, keys, :]) * scale).astype(BF)
            for j in range(4):
                dq[h, rows, HD * j : HD * (j + 1)] = d_query[128 * j : 128 * (j + 1)]
        all_rows = pl.ds(pl.multiple_of(seq * TOK, 128), TOK)
        dkv[h, all_rows, :] = (acc[0] * scale).astype(BF)
        dkv[2 + h, all_rows, :] = acc[1].astype(BF)
        return carry

    lax.fori_loop(0, 4, unit, 0)
    for j in range(4):
        dq[2, :, HD * j : HD * (j + 1)] = dkv[j]
    wait_all(x, sems.at[2])

    def grads(s, carry):
        g[s] = tn(x[...], dq[s]).astype(BF).reshape(64, 32, 512)
        for j, keep, send in ((0, keep0, send0), (1, keep1, send1), (2, keep2, send2)):

            @pl.when(s == j)
            def _():
                def step(p, inner):
                    pltpu.make_async_copy(
                        g.at[j, ids[j, p + 32]], send.at[p], sems.at[3 + j]
                    ).start()
                    pltpu.make_async_copy(
                        g.at[j, ids[j, p]], keep.at[p], sems.at[3 + j]
                    ).start()
                    return inner

                lax.fori_loop(0, 32, step, 0, unroll=4)

        return carry

    lax.fori_loop(0, 3, grads, 0)
    for j in range(3):
        wait_all(g.at[j], sems.at[3 + j])


def backward(ids, x, u, streams, q, kv, col, row):
    return pl.pallas_call(
        backward_body,
        in_specs=[SMEM] + [ANY] * 8 + [VMEM] * 4,
        out_specs=(VMEM,) + (ANY,) * 6,
        out_shape=(jax.ShapeDtypeStruct((64, 16, 2048), BF),) + (HALF,) * 6,
        scratch_shapes=[
            ROWS,
            ROWS,
            pltpu.VMEM((2, 2 * TOK, 512), BF),
            pltpu.VMEM((3, 2 * TOK, 512), BF),
            pltpu.VMEM((4, 2 * TOK, HD), BF),
            pltpu.VMEM((3, 64, 32, 512), BF),
            pltpu.VMEM((2, TOK, HD), F32),
            pltpu.SemaphoreType.DMA((6,)),
        ],
        cost_estimate=cost(2 * 768 * 2048 * 2560, 20 << 20),
        name="back",
    )(ids, *x, *u, *[piece for pair in streams for piece in pair], q, kv, col, row)


def moved(body, ins, outs):
    def kernel(*refs):
        sem = refs[-1]
        copies = [pltpu.make_async_copy(a, b, sem.at[i]) for i, (a, b) in enumerate(body(*refs[:-1]))]
        for copy in copies:
            copy.start()
        for copy in copies:
            copy.wait()

    return pl.pallas_call(
        kernel,
        in_specs=[ANY] * len(ins),
        out_specs=(VMEM,) * len(outs),
        out_shape=outs,
        scratch_shapes=[pltpu.SemaphoreType.DMA((40,))],
    )(*ins)


def joined(blocks):
    n = len(blocks)
    shape = jax.ShapeDtypeStruct((n,) + blocks[0].shape, BF)
    return moved(lambda *r: [(r[i], r[n].at[i]) for i in range(n)], blocks, (shape,))[0]


def by_stream(low, high):
    def pairs(a, b, *outs):
        return [
            (src.at[:, pl.ds(32 * s, 32)], outs[s].at[pl.ds(4 * i, 4)])
            for s in range(5)
            for i, src in enumerate((a, b))
        ]

    shape = jax.ShapeDtypeStruct((8, 32, 512), BF)
    return moved(pairs, (low, high), (shape,) * 5)


def added(a, b):
    return (a.astype(F32) + b.astype(F32)).astype(BF)


def after(x, *deps):
    return lax.optimization_barrier((x, deps))[0]


def late_step(stream, keep, send, stage, *gates):
    recv = across(send, late_links(stream % 3, stage))
    if gates:
        keep = after(keep, *gates)
    n = keep.shape[0] // 2
    if stage == 0:
        return added(keep, recv), None
    return added(keep[:n], recv[:n]), added(keep[n:], recv[n:])


def early_reduce(x):
    total = x[0].astype(F32)
    for recv in [early(x[p], p) for p in range(1, 8)]:
        total = total + recv.astype(F32)
    return total


def adamw(weight, mean_in, square_in, grad):
    new_mean = beta_one * mean_in + (1.0 - beta_one) * grad
    new_square = beta_two * square_in + (1.0 - beta_two) * grad * grad
    corrected = (
        new_mean
        / (1.0 - beta_one**step_count)
        / (jnp.sqrt(new_square / (1.0 - beta_two**step_count)) + epsilon)
    )
    return (weight - learn_rate * (corrected + decay_rate * weight), new_mean, new_square)


def halves(rows):
    return [
        jnp.concatenate(
            [
                rows[:, 1024 * h : 1024 * (h + 1)],
                rows[:, 2048 + 256 * h : 2048 + 256 * (h + 1)],
                rows[:, 2560 + 256 * h : 2560 + 256 * (h + 1)],
            ],
            axis=1,
        )
        for h in range(2)
    ]


def local(
    inputs, upstream, doc_ids, qkv_weight, out_weight, qkv_mean, qkv_square, out_mean, out_square
):
    core = lax.axis_index("dp_2")
    chip = lax.axis_index(("grp", "dp_0", "dp_1"))
    first = core == 0
    ids = jnp.where(first, TABLE[0], TABLE[1]) ^ chip

    h0, h1 = halves(qkv_weight.astype(BF))
    mine, theirs = jnp.where(first, h0, h1), jnp.where(first, h1, h0)
    arrived = to_partner(theirs)
    out_block = lax.ppermute(out_weight.astype(BF), ALL, out_pairs())
    top, bottom = jnp.where(first, mine, arrived), jnp.where(first, arrived, mine)
    block = jnp.concatenate(
        [part[:, 512 * s : 512 * (s + 1)] for s in range(3) for part in (top, bottom)]
        + [out_block[:, 512 * s : 512 * (s + 1)] for s in range(4)],
        axis=0,
    )
    low = joined([block] + [early(block, p) for p in range(1, 4)])
    have = list(by_stream(low, early(low, 4)))

    def gather(s, stage):
        return across(have[s], late_links(s % 3, stage))

    for stage in range(2):
        recv = [gather(s, stage) for s in range(3)]
        have[:3] = [jnp.concatenate(pair, axis=0) for pair in zip(have[:3], recv)]
    streams = [(have[s], gather(s, 2)) for s in range(3)]

    x = (inputs, to_partner(after(inputs, arrived)))
    u = (upstream, to_partner(after(upstream, arrived)))
    docs = jnp.stack([doc_ids, to_partner(after(doc_ids, arrived))])
    col, row = docs.reshape(2 * TOK, 1), docs.reshape(2, 1, TOK)
    x = tuple(normalize(rows) for rows in x)

    for stage in range(2):
        recv = [gather(s, stage) for s in (3, 4)]
        have[3:] = [jnp.concatenate(pair, axis=0) for pair in zip(have[3:], recv)]
    streams += [(have[s], gather(s, 2)) for s in (3, 4)]

    q, kv, mixed, keep3, send3, keep4, send4 = project(
        ids, after(x, have), u, streams[:3], col, row
    )
    out_half, keep0, send0, keep1, send1, keep2, send2 = backward(
        ids, after(x, send3), u, streams[3:], q, kv, col, row
    )
    keep3, send3 = late_step(3, keep3, send3, 2, send2)
    keep4, send4 = late_step(4, keep4, send4, 2, send2)

    out_half = out_half.reshape(1024, 2048)
    mixed = jnp.concatenate([mixed[0], mixed[1]], axis=1)
    mixed = after(mixed, send2, send3, send4)
    other = jnp.dot(mixed[TOK:], out_half, preferred_element_type=F32)
    keep0, send0 = late_step(0, keep0, send0, 2, other)
    keep1, send1 = late_step(1, keep1, send1, 2, other)
    keep2, send2 = late_step(2, keep2, send2, 2, other)
    keep3, send3 = late_step(3, keep3, send3, 1, send2)
    keep4, send4 = late_step(4, keep4, send4, 1, send2)
    own = jnp.dot(after(mixed[:TOK], send3, send4), out_half, preferred_element_type=F32)
    attn_out = (own + to_partner(other)).astype(BF)
    keep0, send0 = late_step(0, keep0, send0, 1, attn_out)
    keep1, send1 = late_step(1, keep1, send1, 1, attn_out)
    keep2, send2 = late_step(2, keep2, send2, 1, attn_out)
    keep3, _ = late_step(3, keep3, send3, 0, send2)
    keep4, _ = late_step(4, keep4, send4, 0, send2)
    keep0, _ = late_step(0, keep0, send0, 0)
    keep1, _ = late_step(1, keep1, send1, 0)
    keep2, _ = late_step(2, keep2, send2, 0)
    total = early_reduce(jnp.concatenate([keep0, keep1, keep2, keep3, keep4], axis=1))
    qkv_sum, out_sum = total[:96], total[96:]

    squares = jnp.sum(qkv_sum * qkv_sum) + jnp.sum(out_sum * out_sum)
    spread = lax.all_to_all(
        jnp.full((128, 128), squares, F32), ALL, split_axis=0, concat_axis=0, tiled=True
    )
    squares = jnp.sum(spread[:, 0])
    rows = qkv_sum.reshape(3, 2, 16, 512)
    mine = jnp.where(first, rows[:, 0], rows[:, 1])
    arrived = to_partner(jnp.where(first, rows[:, 1], rows[:, 0]))
    low, high = jnp.where(first, mine, arrived), jnp.where(first, arrived, mine)
    grad_qkv = jnp.concatenate(
        [low[0], low[1], high[0], high[1]]
        + [low[2, :, :256], high[2, :, :256], low[2, :, 256:], high[2, :, 256:]],
        axis=1,
    )
    back = [(b, a) for a, b in out_pairs()]
    out_rows = jnp.concatenate([out_sum[16 * s : 16 * (s + 1)] for s in range(4)], axis=1)
    grad_out = lax.ppermute(out_rows, ALL, back)

    param_count = 2048 * (3072 + 2048)
    clip = jnp.minimum(1.0, math.sqrt(param_count) / (jnp.sqrt(squares) + 1e-06))
    new_qkv_weight, new_qkv_mean, new_qkv_square = adamw(
        qkv_weight, qkv_mean, qkv_square, clip * grad_qkv
    )
    new_out_weight, new_out_mean, new_out_square = adamw(
        out_weight, out_mean, out_square, clip * grad_out
    )
    return (
        attn_out,
        new_qkv_weight,
        new_out_weight,
        new_qkv_mean,
        new_qkv_square,
        new_out_mean,
        new_out_square,
    )


def solution(mesh):
    finer = Mesh(mesh.devices.reshape(4, 4, 4, 2), ALL)
    wide = P(ALL, None)
    return jax.shard_map(
        local,
        mesh=finer,
        in_specs=(wide, wide, P(ALL), wide, wide, wide, wide, wide, wide),
        out_specs=(wide,) * 7,
        check_vma=False,
    )
```

```python
import math

import jax
import jax.numpy as jnp
import numpy as np
from jax import lax
from jax.experimental import pallas as pl
from jax.experimental.pallas import tpu as pltpu
from jax.sharding import Mesh
from jax.sharding import PartitionSpec as P


HD = 128
TOK = 384
ALL = ("grp", "dp_0", "dp_1", "dp_2")

beta_one = 0.9
beta_two = 0.95
learn_rate = 0.0003
decay_rate = 0.1
epsilon = 1e-08
step_count = 10
norm_eps = 1e-05
masked_score = -1e30
scale = HD ** (-0.5)


MASKS = [(1 if d % 2 == 0 else 3) << (2 * (2 - d // 2)) for d in range(6)]
LATE = ((0, 2, 4), (1, 3, 5))
EARLY = ((1, 3, 5), (0, 2, 4))


def late_links(rotation, stage):
    return tuple(MASKS[LATE[c][(rotation + stage) % 3]] for c in range(2))


def early_mask(core, p):
    m = 0
    for bit in range(3):
        if p >> bit & 1:
            m ^= MASKS[EARLY[core][bit]]
    return m


def block_masks():
    table = np.zeros((2, 3, 64), np.int32)
    for c in range(2):
        for rotation in range(3):
            for p in range(64):
                m = early_mask(c, p)
                for bit in range(3):
                    if p >> (3 + bit) & 1:
                        m ^= MASKS[LATE[c][(rotation + bit) % 3]]
                table[c, rotation, p] = m
    return table


TABLE = block_masks()


def across(x, masks):
    pairs = [((t * 2 + c), ((t ^ masks[c]) * 2 + c)) for t in range(64) for c in range(2)]
    return lax.ppermute(x, ALL, pairs)


def early(x, p):
    return across(x, [early_mask(c, p) for c in range(2)])


def to_partner(x):
    return lax.ppermute(x, "dp_2", [(0, 1), (1, 0)])


def out_pairs():
    pairs = []
    for chip in range(64):
        for c in range(2):
            x = chip >> 4
            target = ((x % 2) * 2 + c) * 16 + (chip & 15)
            pairs.append((chip * 2 + c, target * 2 + x // 2))
    return pairs


def out_row(t):
    xp = t >> 4
    return ((xp >> 1) * 16 + (t & 15)) * 2 + (xp & 1)


def normalize(rows_in):
    values = rows_in.astype(jnp.float32)
    factor = lax.rsqrt(jnp.mean(values * values, axis=-1, keepdims=True) + norm_eps)
    return (values * factor).astype(jnp.bfloat16)


ANY = pl.BlockSpec(memory_space=pl.ANY)
HBM = pl.BlockSpec(memory_space=pltpu.HBM)
SMEM = pl.BlockSpec(memory_space=pltpu.SMEM)
VMEM = pl.BlockSpec(memory_space=pltpu.VMEM)
BF = jnp.bfloat16
F32 = jnp.float32


def cost(flops, nbytes):
    return pl.CostEstimate(flops=flops, bytes_accessed=nbytes, transcendentals=0)


def place_stream(ids, rotation, a, b, w, sem):
    def step(p, carry):
        pltpu.make_async_copy(a.at[p], w.at[ids[rotation, p]], sem).start()
        pltpu.make_async_copy(b.at[p], w.at[ids[rotation, p + 32]], sem).start()
        return carry

    lax.fori_loop(0, 32, step, 0, unroll=8)


def nn(a, b):
    return jnp.dot(a, b, preferred_element_type=F32)


def nt(a, b):
    return lax.dot_general(a, b, (((1,), (1,)), ((), ())), preferred_element_type=F32)


def tn(a, b):
    return lax.dot_general(a, b, (((0,), (0,)), ((), ())), preferred_element_type=F32)


def stacked(ref, g, rows):
    return jnp.concatenate([ref[g, rows, HD * h : HD * (h + 1)] for h in range(4)], axis=0)


def softmax_block(q_ref, kv_ref, col_ref, row_ref, g, seq, i):
    lo, hi = max(0, 128 * (i - 1)), 128 * (i + 1)
    n = hi - lo
    base = seq * TOK
    rows = pl.ds(pl.multiple_of(base + 128 * i, 128), 128)
    keys = pl.ds(pl.multiple_of(base + lo, 128), n)
    q = stacked(q_ref, g, rows)
    scores = nt(q, kv_ref[g, keys, :]) * scale
    t = lax.broadcasted_iota(jnp.int32, (128, n), 0) + 128 * i
    s = lax.broadcasted_iota(jnp.int32, (128, n), 1) + lo
    allowed = (t >= s) & (col_ref[rows, :] == row_ref[seq, :, lo:hi])
    scores = jnp.where(allowed[None], scores.reshape(4, 128, n), masked_score).reshape(512, n)
    exponent = jnp.exp(scores - jnp.max(scores, axis=-1, keepdims=True))
    soft = exponent * (1.0 / jnp.sum(exponent, axis=-1, keepdims=True))
    return q, soft, rows, keys


def load_rows(own, other, dst, sem):
    pltpu.make_async_copy(own, dst.at[pl.ds(0, TOK)], sem).start()
    pltpu.make_async_copy(other, dst.at[pl.ds(TOK, TOK)], sem).start()


def wait_all(ref, sem):
    pltpu.make_async_copy(ref, ref, sem).wait()


def spread_out_rows(ids, half, g, keep, send, sem):
    def step(p, carry):
        pltpu.make_async_copy(g.at[half, ids[3 + half, p + 32]], send.at[p], sem).start()
        pltpu.make_async_copy(g.at[half, ids[3 + half, p]], keep.at[p], sem).start()
        return carry

    lax.fori_loop(0, 32, step, 0, unroll=8)


def project_body(*refs):
    ids, xa, xb, ua, ub, a0, b0, a1, b1, a2, b2, col_ref, row_ref = refs[:13]
    q_out, kv_out, o_out, keep3, send3, keep4, send4 = refs[13:20]
    x, u, w, rows_out, kv_ref, o_ref, g, sems = refs[20:]
    q_ref = rows_out
    pairs = ((a0, b0), (a1, b1), (a2, b2))
    load_rows(xa, xb, x, sems.at[3])
    for s in range(3):
        place_stream(ids, s, *pairs[s], w.at[s], sems.at[s])
    load_rows(ua, ub, u, sems.at[4])
    wait_all(x, sems.at[3])

    def column(s, carry):
        wait_all(w.at[s], sems.at[s])
        rows_out[s] = nn(x[...], w[s].reshape(2048, 512)).astype(BF)
        return carry

    lax.fori_loop(0, 3, column, 0)
    for j in range(4):
        kv_ref[j] = rows_out[2, :, HD * j : HD * (j + 1)]
    copies = [
        pltpu.make_async_copy(a, b, sems.at[7 + i])
        for i, (a, b) in enumerate(
            ((rows_out.at[pl.ds(0, 2)], q_out), (kv_ref, kv_out), (o_ref, o_out))
        )
    ]
    copies[0].start()
    copies[1].start()

    def unit(n, carry):
        h, seq = n // 2, n % 2
        for i in range(3):
            _, soft, rows, keys = softmax_block(q_ref, kv_ref, col_ref, row_ref, h, seq, i)
            mixed = nn(soft.astype(BF), kv_ref[2 + h, keys, :]).astype(BF)
            for j in range(4):
                o_ref[h, rows, HD * j : HD * (j + 1)] = mixed[128 * j : 128 * (j + 1)]
        return carry

    lax.fori_loop(0, 4, unit, 0, unroll=2)
    copies[2].start()
    wait_all(u, sems.at[4])
    for half, keep, send in ((0, keep3, send3), (1, keep4, send4)):

        def group(h, carry):
            out = tn(o_ref[h], u[:, 1024 * half : 1024 * (half + 1)]).astype(BF)
            g[half, pl.ds(32 * h, 32)] = out.reshape(32, 16, 1024)
            return carry

        lax.fori_loop(0, 2, group, 0)
        spread_out_rows(ids, half, g, keep, send, sems.at[5 + half])
    for half in range(2):
        wait_all(g.at[half], sems.at[5 + half])
    for copy in copies:
        copy.wait()


PAIR = jax.ShapeDtypeStruct((2, 2 * TOK, 512), BF)
HALF = jax.ShapeDtypeStruct((32, 32, 512), BF)
WIDE = jax.ShapeDtypeStruct((32, 16, 1024), BF)


ROWS = pltpu.VMEM((2 * TOK, 2048), BF)


def project(ids, x, u, streams, col, row):
    return pl.pallas_call(
        project_body,
        in_specs=[SMEM] + [HBM] * 10 + [VMEM] * 2,
        out_specs=(ANY,) * 7,
        out_shape=(PAIR, jax.ShapeDtypeStruct((4, 2 * TOK, HD), BF), PAIR) + (WIDE,) * 4,
        scratch_shapes=[
            ROWS,
            ROWS,
            pltpu.VMEM((3, 64, 32, 512), BF),
            pltpu.VMEM((3, 2 * TOK, 512), BF),
            pltpu.VMEM((4, 2 * TOK, HD), BF),
            pltpu.VMEM((2, 2 * TOK, 512), BF),
            pltpu.VMEM((2, 64, 16, 1024), BF),
            pltpu.SemaphoreType.DMA((10,)),
        ],
        cost_estimate=cost(2 * 768 * 2048 * 2560, 20 << 20),
        name="project",
    )(ids, *x, *u, *[piece for pair in streams for piece in pair], col, row)


def backward_body(*refs):
    ids, xa, xb, ua, ub, a3, b3, a4, b4, q_ref, kv_ref, col_ref, row_ref = refs[:13]
    w_out, keep0, send0, keep1, send1, keep2, send2 = refs[13:20]
    x, u, w_ref, d_ref, dq, dkv, g, acc, sems = refs[20:]
    load_rows(ua, ub, u, sems.at[0])

    def place(p, carry):
        for half, a, b in ((0, a3, b3), (1, a4, b4)):
            cols = pl.ds(1024 * half, 1024)
            pltpu.make_async_copy(
                a.at[p], w_ref.at[ids[3 + half, p], :, cols], sems.at[1]
            ).start()
            pltpu.make_async_copy(
                b.at[p], w_ref.at[ids[3 + half, p + 32], :, cols], sems.at[1]
            ).start()
        return carry

    lax.fori_loop(0, 32, place, 0, unroll=4)
    load_rows(xa, xb, x, sems.at[2])
    wait_all(u, sems.at[0])
    wait_all(w_ref, sems.at[1])
    w_copy = pltpu.make_async_copy(w_ref, w_out, sems.at[6])
    w_copy.start()

    def heads(h, carry):
        d_ref[h] = nt(u[...], w_ref[pl.ds(32 * h, 32)].reshape(512, 2048)).astype(BF)
        return carry

    lax.fori_loop(0, 2, heads, 0)

    def unit(n, carry):
        h, seq = n // 2, n % 2
        acc[...] = jnp.zeros_like(acc)
        for i in range(3):
            q, soft, rows, keys = softmax_block(q_ref, kv_ref, col_ref, row_ref, h, seq, i)
            own = slice(max(0, 128 * (i - 1)), 128 * (i + 1))
            d_heads = stacked(d_ref, h, rows)
            d_soft = nt(d_heads, kv_ref[2 + h, keys, :])
            delta = jnp.sum(soft * d_soft, axis=-1, keepdims=True)
            d_scores = (soft * (d_soft - delta)).astype(BF)
            acc[1, own, :] += tn(soft.astype(BF), d_heads)
            acc[0, own, :] += tn(d_scores, q)
            d_query = (nn(d_scores, kv_ref[h, keys, :]) * scale).astype(BF)
            for j in range(4):
                dq[h, rows, HD * j : HD * (j + 1)] = d_query[128 * j : 128 * (j + 1)]
        all_rows = pl.ds(pl.multiple_of(seq * TOK, 128), TOK)
        dkv[h, all_rows, :] = (acc[0] * scale).astype(BF)
        dkv[2 + h, all_rows, :] = acc[1].astype(BF)
        return carry

    lax.fori_loop(0, 4, unit, 0)
    for j in range(4):
        dq[2, :, HD * j : HD * (j + 1)] = dkv[j]
    wait_all(x, sems.at[2])

    def grads(s, carry):
        g[s] = tn(x[...], dq[s]).astype(BF).reshape(64, 32, 512)
        for j, keep, send in ((0, keep0, send0), (1, keep1, send1), (2, keep2, send2)):

            @pl.when(s == j)
            def _():
                def step(p, inner):
                    pltpu.make_async_copy(
                        g.at[j, ids[j, p + 32]], send.at[p], sems.at[3 + j]
                    ).start()
                    pltpu.make_async_copy(
                        g.at[j, ids[j, p]], keep.at[p], sems.at[3 + j]
                    ).start()
                    return inner

                lax.fori_loop(0, 32, step, 0, unroll=8)

        return carry

    lax.fori_loop(0, 3, grads, 0)
    for j in range(3):
        wait_all(g.at[j], sems.at[3 + j])
    w_copy.wait()


def backward(ids, x, u, streams, q, kv, col, row):
    return pl.pallas_call(
        backward_body,
        in_specs=[SMEM] + [HBM] * 8 + [VMEM] * 4,
        out_specs=(ANY,) * 7,
        out_shape=(jax.ShapeDtypeStruct((64, 16, 2048), BF),) + (HALF,) * 6,
        scratch_shapes=[
            ROWS,
            ROWS,
            pltpu.VMEM((64, 16, 2048), BF),
            pltpu.VMEM((2, 2 * TOK, 512), BF),
            pltpu.VMEM((3, 2 * TOK, 512), BF),
            pltpu.VMEM((4, 2 * TOK, HD), BF),
            pltpu.VMEM((3, 64, 32, 512), BF),
            pltpu.VMEM((2, TOK, HD), F32),
            pltpu.SemaphoreType.DMA((7,)),
        ],
        cost_estimate=cost(2 * 768 * 2048 * 2560, 20 << 20),
        name="back",
    )(ids, *x, *u, *[piece for pair in streams for piece in pair], q, kv, col, row)


def moved(body, ins, outs):
    def kernel(*refs):
        sem = refs[-1]
        copies = [pltpu.make_async_copy(a, b, sem.at[i]) for i, (a, b) in enumerate(body(*refs[:-1]))]
        for copy in copies:
            copy.start()
        for copy in copies:
            copy.wait()

    return pl.pallas_call(
        kernel,
        in_specs=[HBM] * len(ins),
        out_specs=(VMEM,) * len(outs),
        out_shape=outs,
        scratch_shapes=[pltpu.SemaphoreType.DMA((40,))],
    )(*ins)


def by_stream(pieces):
    def pairs(*refs):
        sources, outs = refs[:4], refs[4:]
        copies = []
        for i, src in enumerate(sources):
            at = pl.ds(2 * i, 2)
            for s in range(3):
                copies.append((src.at[:, pl.ds(32 * s, 32)], outs[s].at[at]))
            for j in range(4):
                target = outs[3 + j // 2].at[at, :, pl.ds(512 * (j % 2), 512)]
                copies.append((src.at[:, pl.ds(96 + 16 * j, 16)], target))
        return copies

    shapes = (jax.ShapeDtypeStruct((8, 32, 512), BF),) * 3
    shapes += (jax.ShapeDtypeStruct((8, 16, 1024), BF),) * 2
    return moved(pairs, pieces, shapes)


def added(a, b):
    return (a.astype(F32) + b.astype(F32)).astype(BF)


def after(x, *deps):
    return lax.optimization_barrier((x, deps))[0]


def late_step(stream, keep, send, stage, *gates):
    recv = across(send, late_links(stream % 3, stage))
    if gates:
        keep = after(keep, *gates)
    n = keep.shape[0] // 2
    if stage == 0:
        return added(keep, recv), None
    return added(keep[:n], recv[:n]), added(keep[n:], recv[n:])


def early_reduce(x):
    total = x[0:2].astype(F32)
    for recv in [early(x[p : p + 2], p) for p in (6, 2, 4)]:
        total = total + recv.astype(F32)
    recv = early(total[1].astype(BF), 1)
    return total[0] + recv.astype(F32)


def adamw(weight, mean_in, square_in, grad):
    new_mean = beta_one * mean_in + (1.0 - beta_one) * grad
    new_square = beta_two * square_in + (1.0 - beta_two) * grad * grad
    corrected = (
        new_mean
        / (1.0 - beta_one**step_count)
        / (jnp.sqrt(new_square / (1.0 - beta_two**step_count)) + epsilon)
    )
    return (weight - learn_rate * (corrected + decay_rate * weight), new_mean, new_square)


def halves(rows):
    return [
        jnp.concatenate(
            [
                rows[:, 1024 * h : 1024 * (h + 1)],
                rows[:, 2048 + 256 * h : 2048 + 256 * (h + 1)],
                rows[:, 2560 + 256 * h : 2560 + 256 * (h + 1)],
            ],
            axis=1,
        )
        for h in range(2)
    ]


def local(
    inputs, upstream, doc_ids, qkv_weight, out_weight, qkv_mean, qkv_square, out_mean, out_square
):
    core = lax.axis_index("dp_2")
    chip = lax.axis_index(("grp", "dp_0", "dp_1"))
    first = core == 0
    ids = jnp.where(first, TABLE[0], TABLE[1]) ^ chip
    ids = jnp.concatenate([ids, out_row(ids[:2])], axis=0)

    h0, h1 = halves(qkv_weight.astype(BF))
    mine, theirs = jnp.where(first, h0, h1), jnp.where(first, h1, h0)
    arrived = to_partner(theirs)
    out_block = lax.ppermute(out_weight.astype(BF), ALL, out_pairs())
    top, bottom = jnp.where(first, mine, arrived), jnp.where(first, arrived, mine)
    block = jnp.concatenate(
        [part[:, 512 * s : 512 * (s + 1)] for s in range(3) for part in (top, bottom)]
        + [out_block[:, 512 * s : 512 * (s + 1)] for s in range(4)],
        axis=0,
    )
    low = jnp.stack([block, early(block, 1)])
    have = list(by_stream([low] + [early(low, p) for p in (2, 4, 6)]))

    def gather(s, stage):
        return across(have[s], late_links(s % 3, stage))

    for stage in range(2):
        recv = [gather(s, stage) for s in range(3)]
        have[:3] = [jnp.concatenate(pair, axis=0) for pair in zip(have[:3], recv)]
    streams = [(have[s], gather(s, 2)) for s in range(3)]

    x = (inputs, to_partner(after(inputs, arrived)))
    u = (upstream, to_partner(after(upstream, arrived)))
    docs = jnp.stack([doc_ids, to_partner(after(doc_ids, arrived))])
    col, row = docs.reshape(2 * TOK, 1), docs.reshape(2, 1, TOK)
    x = tuple(normalize(rows) for rows in x)

    for stage in range(2):
        recv = [gather(s, stage) for s in (3, 4)]
        have[3:] = [jnp.concatenate(pair, axis=0) for pair in zip(have[3:], recv)]
    streams += [(have[s], gather(s, 2)) for s in (3, 4)]

    q, kv, mixed, keep3, send3, keep4, send4 = project(
        ids, after(x, have), u, streams[:3], col, row
    )
    out_half, keep0, send0, keep1, send1, keep2, send2 = backward(
        ids, after(x, send3), u, streams[3:], q, kv, col, row
    )
    keep3, send3 = late_step(3, keep3, send3, 2, send2)
    keep4, send4 = late_step(4, keep4, send4, 2, send2)

    out_half = out_half.reshape(1024, 2048)
    mixed = after(mixed, send2, send3, send4)
    mixed = jnp.concatenate([mixed[0], mixed[1]], axis=1)
    other = jnp.dot(mixed[TOK:], out_half, preferred_element_type=F32)
    keep0, send0 = late_step(0, keep0, send0, 2, other)
    keep1, send1 = late_step(1, keep1, send1, 2, other)
    keep2, send2 = late_step(2, keep2, send2, 2, other)
    keep3, send3 = late_step(3, keep3, send3, 1, send2)
    keep4, send4 = late_step(4, keep4, send4, 1, send2)
    own = jnp.dot(after(mixed[:TOK], send3, send4), out_half, preferred_element_type=F32)
    attn_out = (own + to_partner(other)).astype(BF)
    keep0, send0 = late_step(0, keep0, send0, 1, attn_out)
    keep1, send1 = late_step(1, keep1, send1, 1, attn_out)
    keep2, send2 = late_step(2, keep2, send2, 1, attn_out)
    keep3, _ = late_step(3, keep3, send3, 0, send2)
    keep4, _ = late_step(4, keep4, send4, 0, send2)
    keep0, _ = late_step(0, keep0, send0, 0)
    keep1, _ = late_step(1, keep1, send1, 0)
    keep2, _ = late_step(2, keep2, send2, 0)
    outs = [k[:, :, 512 * j : 512 * (j + 1)] for k in (keep3, keep4) for j in range(2)]
    total = early_reduce(jnp.concatenate([keep0, keep1, keep2] + outs, axis=1))
    qkv_sum, out_sum = total[:96], total[96:]

    squares = jnp.sum((total * total).reshape(160, 4, 128), axis=(0, 1))
    spread = lax.all_to_all(
        jnp.broadcast_to(squares, (128, 128)), ALL, split_axis=0, concat_axis=0, tiled=True
    )
    squares = jnp.sum(spread)
    rows = qkv_sum.reshape(3, 2, 16, 512)
    mine = jnp.where(first, rows[:, 0], rows[:, 1])
    arrived = to_partner(jnp.where(first, rows[:, 1], rows[:, 0]))
    low, high = jnp.where(first, mine, arrived), jnp.where(first, arrived, mine)
    grad_qkv = jnp.concatenate(
        [low[0], low[1], high[0], high[1]]
        + [low[2, :, :256], high[2, :, :256], low[2, :, 256:], high[2, :, 256:]],
        axis=1,
    )
    back = [(b, a) for a, b in out_pairs()]
    out_rows = jnp.concatenate([out_sum[16 * s : 16 * (s + 1)] for s in range(4)], axis=1)
    grad_out = lax.ppermute(out_rows, ALL, back)

    param_count = 2048 * (3072 + 2048)
    clip = jnp.minimum(1.0, math.sqrt(param_count) / (jnp.sqrt(squares) + 1e-06))
    new_qkv_weight, new_qkv_mean, new_qkv_square = adamw(
        qkv_weight, qkv_mean, qkv_square, clip * grad_qkv
    )
    new_out_weight, new_out_mean, new_out_square = adamw(
        out_weight, out_mean, out_square, clip * grad_out
    )
    return (
        attn_out,
        new_qkv_weight,
        new_out_weight,
        new_qkv_mean,
        new_qkv_square,
        new_out_mean,
        new_out_square,
    )


def solution(mesh):
    finer = Mesh(mesh.devices.reshape(4, 4, 4, 2), ALL)
    wide = P(ALL, None)
    return jax.shard_map(
        local,
        mesh=finer,
        in_specs=(wide, wide, P(ALL), wide, wide, wide, wide, wide, wide),
        out_specs=(wide,) * 7,
        check_vma=False,
    )
```

```python
import math

import jax
import jax.numpy as jnp
import numpy as np
from jax import lax
from jax.experimental import pallas as pl
from jax.experimental.pallas import tpu as pltpu
from jax.sharding import Mesh
from jax.sharding import PartitionSpec as P


HD = 128
TOK = 384
ALL = ("grp", "dp_0", "dp_1", "dp_2")

beta_one = 0.9
beta_two = 0.95
learn_rate = 0.0003
decay_rate = 0.1
epsilon = 1e-08
step_count = 10
norm_eps = 1e-05
masked_score = -1e30
scale = HD ** (-0.5)


MASKS = [(1 if d % 2 == 0 else 3) << (2 * (2 - d // 2)) for d in range(6)]
LATE = ((0, 2, 4), (1, 3, 5))
EARLY = ((1, 3, 5), (0, 2, 4))


def late_links(rotation, stage):
    return tuple(MASKS[LATE[c][(rotation + stage) % 3]] for c in range(2))


def early_mask(core, p):
    m = 0
    for bit in range(3):
        if p >> bit & 1:
            m ^= MASKS[EARLY[core][bit]]
    return m


def block_masks():
    table = np.zeros((2, 3, 64), np.int32)
    for c in range(2):
        for rotation in range(3):
            for p in range(64):
                m = early_mask(c, p)
                for bit in range(3):
                    if p >> (3 + bit) & 1:
                        m ^= MASKS[LATE[c][(rotation + bit) % 3]]
                table[c, rotation, p] = m
    return table


TABLE = block_masks()


def across(x, masks):
    pairs = [((t * 2 + c), ((t ^ masks[c]) * 2 + c)) for t in range(64) for c in range(2)]
    return lax.ppermute(x, ALL, pairs)


def early(x, p):
    return across(x, [early_mask(c, p) for c in range(2)])


def to_partner(x):
    return lax.ppermute(x, "dp_2", [(0, 1), (1, 0)])


def out_pairs():
    pairs = []
    for chip in range(64):
        for c in range(2):
            x = chip >> 4
            target = ((x % 2) * 2 + c) * 16 + (chip & 15)
            pairs.append((chip * 2 + c, target * 2 + x // 2))
    return pairs


def out_row(t):
    xp = t >> 4
    return ((xp >> 1) * 16 + (t & 15)) * 2 + (xp & 1)


def normalize(rows_in):
    values = rows_in.astype(jnp.float32)
    factor = lax.rsqrt(jnp.mean(values * values, axis=-1, keepdims=True) + norm_eps)
    return (values * factor).astype(jnp.bfloat16)


ANY = pl.BlockSpec(memory_space=pl.ANY)
HBM = pl.BlockSpec(memory_space=pltpu.HBM)
SMEM = pl.BlockSpec(memory_space=pltpu.SMEM)
VMEM = pl.BlockSpec(memory_space=pltpu.VMEM)
BF = jnp.bfloat16
F32 = jnp.float32


def cost(flops, nbytes):
    return pl.CostEstimate(flops=flops, bytes_accessed=nbytes, transcendentals=0)


def place_stream(ids, rotation, a, b, w, sem):
    def step(p, carry):
        pltpu.make_async_copy(a.at[p], w.at[ids[rotation, p]], sem).start()
        pltpu.make_async_copy(b.at[p], w.at[ids[rotation, p + 32]], sem).start()
        return carry

    lax.fori_loop(0, 32, step, 0, unroll=8)


def nn(a, b):
    return jnp.dot(a, b, preferred_element_type=F32)


def nt(a, b):
    return lax.dot_general(a, b, (((1,), (1,)), ((), ())), preferred_element_type=F32)


def tn(a, b):
    return lax.dot_general(a, b, (((0,), (0,)), ((), ())), preferred_element_type=F32)


def stacked(ref, g, rows):
    return jnp.concatenate([ref[g, rows, HD * h : HD * (h + 1)] for h in range(4)], axis=0)


def softmax_block(q_ref, kv_ref, col_ref, row_ref, g, seq, i):
    lo, hi = max(0, 128 * (i - 1)), 128 * (i + 1)
    n = hi - lo
    base = seq * TOK
    rows = pl.ds(pl.multiple_of(base + 128 * i, 128), 128)
    keys = pl.ds(pl.multiple_of(base + lo, 128), n)
    q = stacked(q_ref, g, rows)
    scores = nt(q, kv_ref[g, keys, :]) * scale
    t = lax.broadcasted_iota(jnp.int32, (128, n), 0) + 128 * i
    s = lax.broadcasted_iota(jnp.int32, (128, n), 1) + lo
    allowed = (t >= s) & (col_ref[rows, :] == row_ref[seq, :, lo:hi])
    scores = jnp.where(allowed[None], scores.reshape(4, 128, n), masked_score).reshape(512, n)
    exponent = jnp.exp(scores - jnp.max(scores, axis=-1, keepdims=True))
    soft = exponent * (1.0 / jnp.sum(exponent, axis=-1, keepdims=True))
    return q, soft, rows, keys


def load_rows(own, other, dst, sem):
    pltpu.make_async_copy(own, dst.at[pl.ds(0, TOK)], sem).start()
    pltpu.make_async_copy(other, dst.at[pl.ds(TOK, TOK)], sem).start()


def wait_all(ref, sem):
    pltpu.make_async_copy(ref, ref, sem).wait()


def spread_out_rows(ids, half, g, keep, send, sem):
    def step(p, carry):
        pltpu.make_async_copy(g.at[half, ids[3 + half, p + 32]], send.at[p], sem).start()
        pltpu.make_async_copy(g.at[half, ids[3 + half, p]], keep.at[p], sem).start()
        return carry

    lax.fori_loop(0, 32, step, 0, unroll=8)


def project_body(*refs):
    ids, xa, xb, ua, ub, a0, b0, a1, b1, a2, b2, col_ref, row_ref = refs[:13]
    q_out, kv_out, o_out, keep3, send3, keep4, send4 = refs[13:20]
    x, u, w, rows_out, kv_ref, o_ref, g, sems = refs[20:]
    q_ref = rows_out
    pairs = ((a0, b0), (a1, b1), (a2, b2))
    load_rows(xa, xb, x, sems.at[3])
    for s in range(3):
        place_stream(ids, s, *pairs[s], w.at[s], sems.at[s])
    load_rows(ua, ub, u, sems.at[4])
    wait_all(x, sems.at[3])

    def column(s, carry):
        wait_all(w.at[s], sems.at[s])
        rows_out[s] = nn(x[...], w[s].reshape(2048, 512)).astype(BF)
        return carry

    lax.fori_loop(0, 3, column, 0)
    for j in range(4):
        kv_ref[j] = rows_out[2, :, HD * j : HD * (j + 1)]
    copies = [
        pltpu.make_async_copy(a, b, sems.at[7 + i])
        for i, (a, b) in enumerate(
            ((rows_out.at[pl.ds(0, 2)], q_out), (kv_ref, kv_out), (o_ref, o_out))
        )
    ]
    copies[0].start()
    copies[1].start()

    def unit(n, carry):
        h, seq = n // 2, n % 2
        for i in range(3):
            _, soft, rows, keys = softmax_block(q_ref, kv_ref, col_ref, row_ref, h, seq, i)
            mixed = nn(soft.astype(BF), kv_ref[2 + h, keys, :]).astype(BF)
            for j in range(4):
                o_ref[h, rows, HD * j : HD * (j + 1)] = mixed[128 * j : 128 * (j + 1)]
        return carry

    lax.fori_loop(0, 4, unit, 0, unroll=2)
    copies[2].start()
    wait_all(u, sems.at[4])
    for half, keep, send in ((0, keep3, send3), (1, keep4, send4)):

        def group(h, carry):
            out = tn(o_ref[h], u[:, 1024 * half : 1024 * (half + 1)]).astype(BF)
            g[half, pl.ds(32 * h, 32)] = out.reshape(32, 16, 1024)
            return carry

        lax.fori_loop(0, 2, group, 0)
        spread_out_rows(ids, half, g, keep, send, sems.at[5 + half])
    for half in range(2):
        wait_all(g.at[half], sems.at[5 + half])
    for copy in copies:
        copy.wait()


PAIR = jax.ShapeDtypeStruct((2, 2 * TOK, 512), BF)
HALF = jax.ShapeDtypeStruct((32, 32, 512), BF)
WIDE = jax.ShapeDtypeStruct((32, 16, 1024), BF)


ROWS = pltpu.VMEM((2 * TOK, 2048), BF)


def project(ids, x, u, streams, col, row):
    return pl.pallas_call(
        project_body,
        in_specs=[SMEM] + [HBM] * 10 + [VMEM] * 2,
        out_specs=(ANY,) * 7,
        out_shape=(PAIR, jax.ShapeDtypeStruct((4, 2 * TOK, HD), BF), PAIR) + (WIDE,) * 4,
        scratch_shapes=[
            ROWS,
            ROWS,
            pltpu.VMEM((3, 64, 32, 512), BF),
            pltpu.VMEM((3, 2 * TOK, 512), BF),
            pltpu.VMEM((4, 2 * TOK, HD), BF),
            pltpu.VMEM((2, 2 * TOK, 512), BF),
            pltpu.VMEM((2, 64, 16, 1024), BF),
            pltpu.SemaphoreType.DMA((10,)),
        ],
        cost_estimate=cost(2 * 768 * 2048 * 2560, 20 << 20),
        name="project",
    )(ids, *x, *u, *[piece for pair in streams for piece in pair], col, row)


def backward_body(*refs):
    ids, xa, xb, ua, ub, a3, b3, a4, b4, q_ref, kv_ref, col_ref, row_ref = refs[:13]
    w_out, keep0, send0, keep1, send1, keep2, send2 = refs[13:20]
    x, u, w_ref, d_ref, dq, dkv, g, acc, sems = refs[20:]
    load_rows(ua, ub, u, sems.at[0])

    def place(p, carry):
        for half, a, b in ((0, a3, b3), (1, a4, b4)):
            cols = pl.ds(1024 * half, 1024)
            pltpu.make_async_copy(
                a.at[p], w_ref.at[ids[3 + half, p], :, cols], sems.at[1]
            ).start()
            pltpu.make_async_copy(
                b.at[p], w_ref.at[ids[3 + half, p + 32], :, cols], sems.at[1]
            ).start()
        return carry

    lax.fori_loop(0, 32, place, 0, unroll=4)
    load_rows(xa, xb, x, sems.at[2])
    wait_all(u, sems.at[0])
    wait_all(w_ref, sems.at[1])
    w_copy = pltpu.make_async_copy(w_ref, w_out, sems.at[6])
    w_copy.start()

    def heads(h, carry):
        d_ref[h] = nt(u[...], w_ref[pl.ds(32 * h, 32)].reshape(512, 2048)).astype(BF)
        return carry

    lax.fori_loop(0, 2, heads, 0)

    def unit(n, carry):
        h, seq = n // 2, n % 2
        acc[...] = jnp.zeros_like(acc)
        for i in range(3):
            q, soft, rows, keys = softmax_block(q_ref, kv_ref, col_ref, row_ref, h, seq, i)
            own = slice(max(0, 128 * (i - 1)), 128 * (i + 1))
            d_heads = stacked(d_ref, h, rows)
            d_soft = nt(d_heads, kv_ref[2 + h, keys, :])
            delta = jnp.sum(soft * d_soft, axis=-1, keepdims=True)
            d_scores = (soft * (d_soft - delta)).astype(BF)
            acc[1, own, :] += tn(soft.astype(BF), d_heads)
            acc[0, own, :] += tn(d_scores, q)
            d_query = (nn(d_scores, kv_ref[h, keys, :]) * scale).astype(BF)
            for j in range(4):
                dq[h, rows, HD * j : HD * (j + 1)] = d_query[128 * j : 128 * (j + 1)]
        all_rows = pl.ds(pl.multiple_of(seq * TOK, 128), TOK)
        dkv[h, all_rows, :] = (acc[0] * scale).astype(BF)
        dkv[2 + h, all_rows, :] = acc[1].astype(BF)
        return carry

    lax.fori_loop(0, 4, unit, 0)
    for j in range(4):
        dq[2, :, HD * j : HD * (j + 1)] = dkv[j]
    wait_all(x, sems.at[2])

    def grads(s, carry):
        g[s] = tn(x[...], dq[s]).astype(BF).reshape(64, 32, 512)
        for j, keep, send in ((0, keep0, send0), (1, keep1, send1), (2, keep2, send2)):

            @pl.when(s == j)
            def _():
                def step(p, inner):
                    pltpu.make_async_copy(
                        g.at[j, ids[j, p + 32]], send.at[p], sems.at[3 + j]
                    ).start()
                    pltpu.make_async_copy(
                        g.at[j, ids[j, p]], keep.at[p], sems.at[3 + j]
                    ).start()
                    return inner

                lax.fori_loop(0, 32, step, 0, unroll=8)

        return carry

    lax.fori_loop(0, 3, grads, 0)
    for j in range(3):
        wait_all(g.at[j], sems.at[3 + j])
    w_copy.wait()


def backward(ids, x, u, streams, q, kv, col, row):
    return pl.pallas_call(
        backward_body,
        in_specs=[SMEM] + [HBM] * 8 + [VMEM] * 4,
        out_specs=(ANY,) * 7,
        out_shape=(jax.ShapeDtypeStruct((64, 16, 2048), BF),) + (HALF,) * 6,
        scratch_shapes=[
            ROWS,
            ROWS,
            pltpu.VMEM((64, 16, 2048), BF),
            pltpu.VMEM((2, 2 * TOK, 512), BF),
            pltpu.VMEM((3, 2 * TOK, 512), BF),
            pltpu.VMEM((4, 2 * TOK, HD), BF),
            pltpu.VMEM((3, 64, 32, 512), BF),
            pltpu.VMEM((2, TOK, HD), F32),
            pltpu.SemaphoreType.DMA((7,)),
        ],
        cost_estimate=cost(2 * 768 * 2048 * 2560, 20 << 20),
        name="back",
    )(ids, *x, *u, *[piece for pair in streams for piece in pair], q, kv, col, row)


def moved(body, ins, outs):
    def kernel(*refs):
        sem = refs[-1]
        copies = [pltpu.make_async_copy(a, b, sem.at[i]) for i, (a, b) in enumerate(body(*refs[:-1]))]
        for copy in copies:
            copy.start()
        for copy in copies:
            copy.wait()

    return pl.pallas_call(
        kernel,
        in_specs=[HBM] * len(ins),
        out_specs=(VMEM,) * len(outs),
        out_shape=outs,
        scratch_shapes=[pltpu.SemaphoreType.DMA((40,))],
    )(*ins)


def qkv_streams(pieces):
    def pairs(*refs):
        return [
            (src.at[:, pl.ds(32 * s, 32)], refs[4 + s].at[pl.ds(2 * i, 2)])
            for i, src in enumerate(refs[:4])
            for s in range(3)
        ]

    return moved(pairs, pieces, (jax.ShapeDtypeStruct((8, 32, 512), BF),) * 3)


def out_streams(pieces):
    def pairs(*refs):
        return [
            (
                src.at[:, pl.ds(96 + 16 * j, 16)],
                refs[4 + j // 2].at[pl.ds(2 * i, 2), :, pl.ds(512 * (j % 2), 512)],
            )
            for i, src in enumerate(refs[:4])
            for j in range(4)
        ]

    return moved(pairs, pieces, (jax.ShapeDtypeStruct((8, 16, 1024), BF),) * 2)


def added(a, b):
    return (a.astype(F32) + b.astype(F32)).astype(BF)


def after(x, *deps):
    return lax.optimization_barrier((x, deps))[0]


def late_step(stream, keep, send, stage, *gates):
    recv = across(send, late_links(stream % 3, stage))
    if gates:
        keep = after(keep, *gates)
    n = keep.shape[0] // 2
    if stage == 0:
        return added(keep, recv), None
    return added(keep[:n], recv[:n]), added(keep[n:], recv[n:])


def early_reduce(x):
    total = x[0:2].astype(F32)
    for recv in [early(x[p : p + 2], p) for p in (6, 2, 4)]:
        total = total + recv.astype(F32)
    recv = early(total[1].astype(BF), 1)
    return total[0] + recv.astype(F32)


def adamw(weight, mean_in, square_in, grad):
    new_mean = beta_one * mean_in + (1.0 - beta_one) * grad
    new_square = beta_two * square_in + (1.0 - beta_two) * grad * grad
    corrected = (
        new_mean
        / (1.0 - beta_one**step_count)
        / (jnp.sqrt(new_square / (1.0 - beta_two**step_count)) + epsilon)
    )
    return (weight - learn_rate * (corrected + decay_rate * weight), new_mean, new_square)


def halves(rows):
    return [
        jnp.concatenate(
            [
                rows[:, 1024 * h : 1024 * (h + 1)],
                rows[:, 2048 + 256 * h : 2048 + 256 * (h + 1)],
                rows[:, 2560 + 256 * h : 2560 + 256 * (h + 1)],
            ],
            axis=1,
        )
        for h in range(2)
    ]


def local(
    inputs, upstream, doc_ids, qkv_weight, out_weight, qkv_mean, qkv_square, out_mean, out_square
):
    core = lax.axis_index("dp_2")
    chip = lax.axis_index(("grp", "dp_0", "dp_1"))
    first = core == 0
    ids = jnp.where(first, TABLE[0], TABLE[1]) ^ chip
    ids = jnp.concatenate([ids, out_row(ids[:2])], axis=0)

    h0, h1 = halves(qkv_weight.astype(BF))
    mine, theirs = jnp.where(first, h0, h1), jnp.where(first, h1, h0)
    arrived = to_partner(theirs)
    out_block = lax.ppermute(out_weight.astype(BF), ALL, out_pairs())
    top, bottom = jnp.where(first, mine, arrived), jnp.where(first, arrived, mine)
    block = jnp.concatenate(
        [part[:, 512 * s : 512 * (s + 1)] for s in range(3) for part in (top, bottom)]
        + [out_block[:, 512 * s : 512 * (s + 1)] for s in range(4)],
        axis=0,
    )
    low = jnp.stack([block, early(block, 1)])
    pieces = [low] + [early(low, p) for p in (2, 4, 6)]
    have = list(qkv_streams(pieces))
    have += out_streams(pieces)

    def gather(s, stage):
        return across(have[s], late_links(s % 3, stage))

    for stage in range(2):
        recv = [gather(s, stage) for s in range(3)]
        have[:3] = [jnp.concatenate(pair, axis=0) for pair in zip(have[:3], recv)]
    streams = [(have[s], gather(s, 2)) for s in range(3)]

    x = (inputs, to_partner(after(inputs, arrived)))
    u = (upstream, to_partner(after(upstream, arrived)))
    docs = jnp.stack([doc_ids, to_partner(after(doc_ids, arrived))])
    col, row = docs.reshape(2 * TOK, 1), docs.reshape(2, 1, TOK)
    x = tuple(normalize(rows) for rows in x)

    for stage in range(2):
        recv = [gather(s, stage) for s in (3, 4)]
        have[3:] = [jnp.concatenate(pair, axis=0) for pair in zip(have[3:], recv)]
    streams += [(have[s], gather(s, 2)) for s in (3, 4)]

    q, kv, mixed, keep3, send3, keep4, send4 = project(
        ids, after(x, have), u, streams[:3], col, row
    )
    out_half, keep0, send0, keep1, send1, keep2, send2 = backward(
        ids, after(x, send3), u, streams[3:], q, kv, col, row
    )
    keep3, send3 = late_step(3, keep3, send3, 2, send2)
    keep4, send4 = late_step(4, keep4, send4, 2, send2)

    out_half = out_half.reshape(1024, 2048)
    mixed = after(mixed, send2, send3, send4)
    mixed = jnp.concatenate([mixed[0], mixed[1]], axis=1)
    other = jnp.dot(mixed[TOK:], out_half, preferred_element_type=F32)
    keep0, send0 = late_step(0, keep0, send0, 2, other)
    keep1, send1 = late_step(1, keep1, send1, 2, other)
    keep2, send2 = late_step(2, keep2, send2, 2, other)
    keep3, send3 = late_step(3, keep3, send3, 1, send2)
    keep4, send4 = late_step(4, keep4, send4, 1, send2)
    own = jnp.dot(after(mixed[:TOK], send3, send4), out_half, preferred_element_type=F32)
    attn_out = (own + to_partner(other)).astype(BF)
    keep0, send0 = late_step(0, keep0, send0, 1, attn_out)
    keep1, send1 = late_step(1, keep1, send1, 1, attn_out)
    keep2, send2 = late_step(2, keep2, send2, 1, attn_out)
    keep3, _ = late_step(3, keep3, send3, 0, send2)
    keep4, _ = late_step(4, keep4, send4, 0, send2)
    keep0, _ = late_step(0, keep0, send0, 0)
    keep1, _ = late_step(1, keep1, send1, 0)
    keep2, _ = late_step(2, keep2, send2, 0)
    outs = [k[:, :, 512 * j : 512 * (j + 1)] for k in (keep3, keep4) for j in range(2)]
    total = early_reduce(jnp.concatenate([keep0, keep1, keep2] + outs, axis=1))
    qkv_sum, out_sum = total[:96], total[96:]

    squares = jnp.sum((total * total).reshape(160, 4, 128), axis=(0, 1))
    spread = lax.all_to_all(
        jnp.broadcast_to(squares, (128, 128)), ALL, split_axis=0, concat_axis=0, tiled=True
    )
    squares = jnp.sum(spread)
    rows = qkv_sum.reshape(3, 2, 16, 512)
    mine = jnp.where(first, rows[:, 0], rows[:, 1])
    arrived = to_partner(jnp.where(first, rows[:, 1], rows[:, 0]))
    low, high = jnp.where(first, mine, arrived), jnp.where(first, arrived, mine)
    grad_qkv = jnp.concatenate(
        [low[0], low[1], high[0], high[1]]
        + [low[2, :, :256], high[2, :, :256], low[2, :, 256:], high[2, :, 256:]],
        axis=1,
    )
    back = [(b, a) for a, b in out_pairs()]
    out_rows = jnp.concatenate([out_sum[16 * s : 16 * (s + 1)] for s in range(4)], axis=1)
    grad_out = lax.ppermute(out_rows, ALL, back)

    param_count = 2048 * (3072 + 2048)
    clip = jnp.minimum(1.0, math.sqrt(param_count) / (jnp.sqrt(squares) + 1e-06))
    new_qkv_weight, new_qkv_mean, new_qkv_square = adamw(
        qkv_weight, qkv_mean, qkv_square, clip * grad_qkv
    )
    new_out_weight, new_out_mean, new_out_square = adamw(
        out_weight, out_mean, out_square, clip * grad_out
    )
    return (
        attn_out,
        new_qkv_weight,
        new_out_weight,
        new_qkv_mean,
        new_qkv_square,
        new_out_mean,
        new_out_square,
    )


def solution(mesh):
    finer = Mesh(mesh.devices.reshape(4, 4, 4, 2), ALL)
    wide = P(ALL, None)
    return jax.shard_map(
        local,
        mesh=finer,
        in_specs=(wide, wide, P(ALL), wide, wide, wide, wide, wide, wide),
        out_specs=(wide,) * 7,
        check_vma=False,
    )
```
